256 devices in a mesh: row: 4 (over y_lo, core), phi: 64 (over x, y_hi, z).
Axes of the slice: x: 4, y: 4 (y_hi: 2, y_lo: 2; y = y_hi * 2 + y_lo), z: 8, core: 2. Of those that a mesh axis runs over, the one named last changes fastest.
Arguments:
- hydro_vars: float32 [5, 128, 1024, 256], P(None, 'row', 'phi'), may hold values from -6 to 6
- face_b: float32 [3, 128, 1024, 256], P(None, 'row', 'phi'), may hold values from -6 to 6
- widths: int32 [16], replicated, may hold values from 2 to 1024, as said below
- diffusion: float32 [5, 256], replicated, may hold values from 0.01 to 0.06
Outputs:
- conserved: float32 [8, 128, 1024, 256], P(None, 'row', 'phi')
- faces_out: float32 [3, 128, 1024, 256], P(None, 'row', 'phi')
The draws below stay inside these ranges and needn't reach their ends.
Inputs may be any that keep to these rules, and one draw needn't show every extreme that they name: `widths`: every width is a power of two that divides 1024; the two cycles next to the poles (entries 0 and 15) use 1024.
All inputs are finite; a program needn't handle non-finite values.
Results may differ from the reference program's by a relative error of at most 0.0001.
Values sent between devices are 32-bit elements; how exact they have to be, the bound alone decides.
A program may use at most 64 MiB of HBM per device.

```python
import math
import jax
import jax.numpy as jnp
from jax import lax

NTH = 256
CYCLES = 8
NR = 128
PHI_CELLS = 1024


def draw_widths(key, part):
    top = PHI_CELLS.bit_length() - 1
    powers = jax.random.randint(jax.random.fold_in(key, 7), (2 * CYCLES,), 1, top + 1)
    powers = powers.at[0].set(top).at[2 * CYCLES - 1].set(top)
    return jnp.power(2, powers).astype(jnp.int32)


def block_scale(rng, extent, pieces, low, high):
    loudness, own = 1.0, jax.random.fold_in(rng, 6)
    for position, blocks in pieces:
        draws = jnp.exp(jax.random.uniform(jax.random.fold_in(own, position), (blocks,), jnp.float32, low / len(pieces), high / len(pieces)))
        loudness = loudness * jnp.repeat(draws, extent[position] // blocks).reshape([-1 if axis == position else 1 for axis in range(len(extent))])
    return loudness


def centred(rng, extent, scale, limit, cuts=(), kind=jnp.bfloat16):
    values = jax.random.normal(rng, extent, jnp.float32) * scale
    if len(cuts) > 0:
        values = block_scale(rng, extent, cuts, -0.22, 0.18) * values
    return jnp.clip(values, min=-limit, max=limit).astype(kind)


def setup_inputs(seed: int = 0) -> dict:
    key_of = jax.random.split(jax.random.key(seed), 5)
    hydro_vars = centred(key_of[0], (5, NR, PHI_CELLS, NTH), 1.0, 6.0, ((1, 4), (2, 64)), jnp.float32)
    face_b = centred(key_of[1], (3, NR, PHI_CELLS, NTH), 1.0, 6.0, ((1, 4), (2, 64)), jnp.float32)
    widths = draw_widths(jax.random.fold_in(key_of[4], 71), 0)
    diffusion = jnp.clip(jnp.exp(jax.random.uniform(key_of[3], (5, NTH), jnp.float32, math.log(0.01), math.log(0.06))), 0.01, 0.06)
    return dict(hydro_vars=hydro_vars, face_b=face_b, widths=widths, diffusion=diffusion)


def stencil(padded, axis, count):
    parts = [lax.slice_in_dim(padded, offset, offset + count, axis=axis) for offset in range(5)]
    return (16.0 * (parts[1] + parts[3]) - (parts[0] + parts[4]) - 30.0 * parts[2]) / 12.0


def fourth(values, axis, wrapped):
    count = values.shape[axis]
    pads = [(0, 0)] * values.ndim
    pads[axis] = (2, 2)
    padded = jnp.pad(values, pads, mode="wrap") if wrapped else jnp.pad(values, pads)
    return stencil(padded, axis, count)


def block_means(cycles, axis, width):
    cells = cycles.shape[axis]
    result = cycles
    for power in range(1, cells.bit_length()):
        size = 2 ** power
        shape = cycles.shape[:axis] + (cells // size, size) + cycles.shape[axis + 1:]
        means = jnp.mean(cycles.reshape(shape), axis=axis + 1, keepdims=True)
        means = jnp.broadcast_to(means, shape).reshape(cycles.shape)
        result = jnp.where(width == size, means, result)
    return result


def reference(hydro_vars, face_b, widths, diffusion):
    fields = jnp.concatenate([hydro_vars, face_b], 0)
    theta_cells = fields.shape[3]
    polar_cycles = jnp.concatenate([fields[..., :CYCLES], fields[..., theta_cells - CYCLES:]], 3)
    averaged = block_means(polar_cycles, 2, widths)
    fields = jnp.concatenate([averaged[..., :CYCLES], fields[..., CYCLES:theta_cells - CYCLES], averaged[..., CYCLES:]], 3)
    hydro = fields[:5]
    change = fourth(hydro, 1, False) + fourth(hydro, 2, True) + fourth(hydro, 3, False)
    smoothed = hydro + diffusion[:, None, None, :] * change
    radial = fields[5]
    polar_face = fields[6]
    azimuth = fields[7]
    radial_next = jnp.concatenate([radial[1:], jnp.zeros_like(radial[:1])], 0)
    polar_next = jnp.concatenate([polar_face[..., 1:], jnp.zeros_like(polar_face[..., :1])], 2)
    azimuth_next = jnp.roll(azimuth, -1, axis=1)
    cell_field = 0.5 * jnp.stack([radial + radial_next, polar_face + polar_next, azimuth + azimuth_next])
    return jnp.concatenate([smoothed, cell_field], 0), fields[5:]
```

```python
import jax
import jax.numpy as jnp
from jax import lax
from jax.experimental import pallas as pl
from jax.experimental.pallas import tpu as pltpu
from jax.sharding import PartitionSpec as P

F32 = jnp.float32
MESH = pl.DeviceIdType.MESH
NV, NF, FIELDS = 5, 3, 8
ROWS, CELLS, THETA = 32, 16, 256
NZ, NG, NROW = 8, 8, 4
EARLY = 2
FAR_FIRST = (4, 3, 5, 2, 6, 1, 7)


def lanes(shape):
    return lax.broadcasted_iota(jnp.int32, shape, len(shape) - 1)


def sublanes(shape):
    return lax.broadcasted_iota(jnp.int32, shape, len(shape) - 2)


def exchange(
    widths, hydro, face, halo, radial, polar,
    hv, fv, la, zsum, gsum, edge, first, last, first_in, last_in, la_in,
    load_sem, q_send, q_recv, qn_send, qn_recv, qp_send, qp_recv,
    la_send, la_recv, e_send, e_recv, g_send, g_recv,
    p_send, p_recv, r_send, r_recv,
):
    row, phi = lax.axis_index("row"), lax.axis_index("phi")
    z, g = phi % NZ, phi // NZ
    nphi = NZ * NG
    after, before = (phi + 1) % nphi, (phi + nphi - 1) % nphi
    has_prev, has_next = row > 0, row < NROW - 1

    def peer(d):
        return g * NZ + (z + d) % NZ

    def group(d):
        return ((g + d) % NG) * NZ + z

    loads = [pltpu.make_async_copy(hydro.at[i], hv.at[i], load_sem.at[i]) for i in range(NV)]
    loads += [pltpu.make_async_copy(face.at[i], fv.at[i], load_sem.at[NV + i]) for i in range(NF)]
    for copy in loads:
        copy.start()

    zsum[:, ROWS:, :] = jnp.zeros((NZ, 8, 128), F32)
    barrier = pltpu.get_barrier_semaphore()

    def hello(r, p):
        pl.semaphore_signal(barrier, inc=1, device_id=(r, p), device_id_type=MESH)

    for d in range(1, NZ):
        hello(row, peer(d))
        hello(row, group(d))

    @pl.when(has_prev)
    def _():
        for d in range(NZ):
            hello(row - 1, peer(d))

    @pl.when(has_next)
    def _():
        for d in range(NZ):
            hello(row + 1, peer(d))

    @pl.when(z == 0)
    def _():
        hello(row, before)

    @pl.when(z == NZ - 1)
    def _():
        hello(row, after)

    lane = lanes((8, 128))
    sub = sublanes((8, 128))
    width = jnp.zeros((8, 128), jnp.int32)
    for c in range(16):
        width = jnp.where(lane % 16 == c, widths[(c + 8) % 16], width)
    low = lane < 64

    for copy in loads:
        copy.wait()

    def pack(block, carry):
        q8 = jnp.zeros((8, 128), F32)
        f8 = jnp.zeros((8, 128), F32)
        l8 = jnp.zeros((8, 128), F32)
        for i in range(8):
            r = block * 8 + i
            parts = []
            for j in range(2):
                packed = None
                for f in range(FIELDS):
                    ref, k = (hv, f) if f < NV else (fv, f - NV)
                    t0 = ref[k, r, 8 * j:8 * j + 8, 0:128]
                    t1 = ref[k, r, 8 * j:8 * j + 8, 128:256]
                    t = pltpu.roll(jnp.where(low, t0, t1), (8 + 16 * f) % 128, 1)
                    packed = t if packed is None else jnp.where(lane // 16 == f, t, packed)
                parts.append(packed)
            sums, local = [], []
            for p in parts:
                s2 = p + jnp.where(sub % 2 == 0, pltpu.roll(p, 7, 0), pltpu.roll(p, 1, 0))
                s4 = s2 + jnp.where(sub % 4 < 2, pltpu.roll(s2, 6, 0), pltpu.roll(s2, 2, 0))
                s8 = s4 + pltpu.roll(s4, 4, 0)
                sums.append(s8)
                local.append((s2, s4, s8))
            s16 = sums[0] + sums[1]
            for j, (s2, s4, s8) in enumerate(local):
                mean = jnp.where(width == 2, s2 * 0.5, s16 * 0.0625)
                mean = jnp.where(width == 4, s4 * 0.25, mean)
                mean = jnp.where(width == 8, s8 * 0.125, mean)
                la[r, 8 * j:8 * j + 8, :] = mean
                local[j] = mean
            q8 = jnp.where(sub == i, s16, q8)
            f8 = jnp.where(sub == i, pltpu.roll(local[0], i, 0) if i else local[0], f8)
            l8 = jnp.where(sub == i, pltpu.roll(local[1], (i + 1) % 8, 0) if i < 7 else local[1], l8)
        at = pl.ds(pl.multiple_of(block * 8, 8), 8)
        zsum[z, at, :] = q8
        first[at, :] = f8
        last[at, :] = l8
        return carry

    lax.fori_loop(0, ROWS // 8, pack, 0)

    hellos = 2 * (NZ - 1) + NZ * (has_prev.astype(jnp.int32) + has_next.astype(jnp.int32))
    hellos += (z == 0).astype(jnp.int32) + (z == NZ - 1).astype(jnp.int32)
    pl.semaphore_wait(barrier, hellos)

    def remote(src, dst, ssem, rsem, r, p):
        return pltpu.make_async_remote_copy(
            src_ref=src, dst_ref=dst, send_sem=ssem, recv_sem=rsem,
            device_id=(r, p), device_id_type=MESH,
        )

    def q_copy(d):
        ref = zsum.at[z, 0:ROWS, :]
        return remote(ref, ref, q_send.at[d], q_recv.at[d], row, peer(d))

    def q_down(d):
        return remote(
            zsum.at[z, 0:2, :], zsum.at[z, ROWS + 2:ROWS + 4, :],
            qn_send.at[d], qn_recv.at[d], row - 1, peer(d),
        )

    def q_up(d):
        return remote(
            zsum.at[z, ROWS - 2:ROWS, :], zsum.at[z, ROWS:ROWS + 2, :],
            qp_send.at[d], qp_recv.at[d], row + 1, peer(d),
        )

    for d in FAR_FIRST:
        q_copy(d).start()

    @pl.when(has_prev)
    def _():
        for d in FAR_FIRST + (0,):
            q_down(d).start()

    @pl.when(has_next)
    def _():
        for d in FAR_FIRST + (0,):
            q_up(d).start()

    edge_first = remote(first, first_in, la_send.at[0], la_recv.at[0], row, before)
    edge_last = remote(last, last_in, la_send.at[1], la_recv.at[1], row, after)
    edge_first.start()
    edge_last.start()
    la_down = remote(la.at[0:2], la_in.at[2:4], la_send.at[2], la_recv.at[2], row - 1, phi)
    la_up = remote(la.at[ROWS - 2:ROWS], la_in.at[0:2], la_send.at[3], la_recv.at[3], row + 1, phi)

    down = [remote(hv.at[:, 0:2], radial.at[0:NV, 2:4], r_send.at[0], r_recv.at[0], row - 1, phi)]
    down += [remote(fv.at[0, 0:1], radial.at[NV, 2:3], r_send.at[1], r_recv.at[1], row - 1, phi)]
    up = [remote(hv.at[:, ROWS - 2:ROWS], radial.at[0:NV, 0:2], r_send.at[2], r_recv.at[2], row + 1, phi)]

    @pl.when(has_prev)
    def _():
        la_down.start()
        for copy in down:
            copy.start()

    @pl.when(has_next)
    def _():
        la_up.start()
        for copy in up:
            copy.start()

    bulk = []
    for i in range(NV):
        bulk.append(remote(
            hv.at[i, :, CELLS - 2:CELLS, :], halo.at[i, :, 6:8, :],
            p_send.at[2 * i], p_recv.at[2 * i], row, after,
        ))
        bulk.append(remote(
            hv.at[i, :, 0:2, :], halo.at[i, :, 0:2, :],
            p_send.at[2 * i + 1], p_recv.at[2 * i + 1], row, before,
        ))
    bulk.append(remote(
        fv.at[2, :, 0:1, :], halo.at[NV, :, 0:1, :],
        p_send.at[2 * NV], p_recv.at[2 * NV], row, before,
    ))
    for copy in bulk[:2 * EARLY]:
        copy.start()

    for d in FAR_FIRST:
        q_copy(d).wait_recv()

    @pl.when(has_prev)
    def _():
        for d in FAR_FIRST + (0,):
            q_up(d).wait_recv()

    @pl.when(has_next)
    def _():
        for d in FAR_FIRST + (0,):
            q_down(d).wait_recv()

    def z_sums(at):
        pair, quad = (at // 2) * 2, (at // 4) * 4
        s32 = zsum[pair] + zsum[pair + 1]
        s64 = (zsum[quad] + zsum[quad + 1]) + (zsum[quad + 2] + zsum[quad + 3])
        return s32, s64

    tall = (ROWS + 8, 128)
    width = jnp.broadcast_to(width[0:1], tall)
    total = zsum[0]
    for i in range(1, NZ):
        total = total + zsum[i]
    gsum[g] = total

    def g_copy(d):
        return remote(gsum.at[g], gsum.at[g], g_send.at[d], g_recv.at[d], row, group(d))

    for d in (5, 3, 7, 1, 6, 2, 4):
        g_copy(d).start()

    s32, s64 = z_sums(z)
    small = jnp.where(width == 32, s32 * (1 / 32), s64 * (1 / 64))
    s32p, s64p = z_sums((z + NZ - 1) % NZ)
    s32n, s64n = z_sums((z + 1) % NZ)
    edge[0] = jnp.where(width == 32, s32p * (1 / 32), s64p * (1 / 64))[:ROWS]
    edge[1] = jnp.where(width == 32, s32n * (1 / 32), s64n * (1 / 64))[:ROWS]
    edge_up = remote(edge.at[0], edge.at[2], e_send.at[0], e_recv.at[0], row, group(1))
    edge_down = remote(edge.at[1], edge.at[3], e_send.at[1], e_recv.at[1], row, group(NG - 1))

    edge_up.start()
    edge_down.start()

    for copy in bulk[2 * EARLY:]:
        copy.start()

    for d in (5, 3, 7, 1, 6, 2, 4):
        g_copy(d).wait_recv()
    edge_up.wait_recv()
    edge_down.wait_recv()
    edge_first.wait_recv()
    edge_last.wait_recv()

    def g_means(at, small):
        pair, quad = (at // 2) * 2, (at // 4) * 4
        mean = jnp.where(width == 128, gsum[at] * (1 / 128), small)
        mean = jnp.where(width == 256, (gsum[pair] + gsum[pair + 1]) * (1 / 256), mean)
        four = (gsum[quad] + gsum[quad + 1]) + (gsum[quad + 2] + gsum[quad + 3])
        mean = jnp.where(width == 512, four * (1 / 512), mean)
        whole = gsum[0]
        for i in range(1, NG):
            whole = whole + gsum[i]
        return jnp.where(width == 1024, whole * (1 / 1024), mean)

    mean = g_means(g, small)
    gp = jnp.where(z == 0, (g + NG - 1) % NG, g)
    gn = jnp.where(z == NZ - 1, (g + 1) % NG, g)
    pad = jnp.zeros((8, 128), F32)
    ep = jnp.concatenate([jnp.where(z == 0, edge[2], edge[0]), pad])
    en = jnp.concatenate([jnp.where(z == NZ - 1, edge[3], edge[1]), pad])
    mean_p = jnp.where(width <= 16, jnp.concatenate([last_in[...], pad]), g_means(gp, ep))
    mean_n = jnp.where(width <= 16, jnp.concatenate([first_in[...], pad]), g_means(gn, en))
    narrow = jnp.broadcast_to(width[0:1], (CELLS, 128)) <= 16
    for r in range(ROWS):
        polar[r, 0:CELLS, :] = jnp.where(narrow, la[r], mean[r:r + 1])
        polar[r, CELLS:, :] = jnp.where(sub < 4, mean_n[r:r + 1], mean_p[r:r + 1])

    @pl.when(has_prev)
    def _():
        la_up.wait_recv()

    @pl.when(has_next)
    def _():
        la_down.wait_recv()

    for i in range(4):
        r = ROWS + i
        polar[r, 0:CELLS, :] = jnp.where(narrow, la_in[i], mean[r:r + 1])
        polar[r, CELLS:, :] = jnp.zeros((8, 128), F32)

    for copy in bulk:
        copy.wait_recv()

    @pl.when(has_prev)
    def _():
        for copy in up:
            copy.wait_recv()

    @pl.when(has_next)
    def _():
        for copy in down:
            copy.wait_recv()

    for d in FAR_FIRST:
        q_copy(d).wait_send()
        g_copy(d).wait_send()
    for copy in bulk + [edge_up, edge_down, edge_first, edge_last]:
        copy.wait_send()

    @pl.when(has_prev)
    def _():
        la_down.wait_send()
        for copy in down:
            copy.wait_send()
        for d in range(NZ):
            q_down(d).wait_send()

    @pl.when(has_next)
    def _():
        la_up.wait_send()
        for copy in up:
            copy.wait_send()
        for d in range(NZ):
            q_up(d).wait_send()


def run_exchange(widths, hydro, face):
    dma = pltpu.SemaphoreType.DMA
    return pl.pallas_call(
        exchange,
        out_shape=(
            jax.ShapeDtypeStruct((NV + 1, ROWS, 8, THETA), F32),
            jax.ShapeDtypeStruct((NV + 1, 4, CELLS, THETA), F32),
            jax.ShapeDtypeStruct((ROWS + 4, CELLS + 8, 128), F32),
        ),
        in_specs=[
            pl.BlockSpec(memory_space=pltpu.SMEM),
            pl.BlockSpec(memory_space=pl.ANY),
            pl.BlockSpec(memory_space=pl.ANY),
        ],
        out_specs=(
            pl.BlockSpec(memory_space=pl.ANY),
            pl.BlockSpec(memory_space=pl.ANY),
            pl.BlockSpec(memory_space=pltpu.VMEM),
        ),
        scratch_shapes=[
            pltpu.VMEM((NV, ROWS, CELLS, THETA), F32),
            pltpu.VMEM((NF, ROWS, CELLS, THETA), F32),
            pltpu.VMEM((ROWS, CELLS, 128), F32),
            pltpu.VMEM((NZ, ROWS + 8, 128), F32),
            pltpu.VMEM((NG, ROWS + 8, 128), F32),
            pltpu.VMEM((4, ROWS, 128), F32),
            pltpu.VMEM((ROWS, 128), F32),
            pltpu.VMEM((ROWS, 128), F32),
            pltpu.VMEM((ROWS, 128), F32),
            pltpu.VMEM((ROWS, 128), F32),
            pltpu.VMEM((4, CELLS, 128), F32),
            dma((FIELDS,)),
            dma((NZ,)), dma((NZ,)), dma((NZ,)), dma((NZ,)), dma((NZ,)), dma((NZ,)),
            dma((4,)), dma((4,)), dma((2,)), dma((2,)), dma((NG,)), dma((NG,)),
            dma((2 * NV + 1,)), dma((2 * NV + 1,)), dma((3,)), dma((3,)),
        ],
        compiler_params=pltpu.CompilerParams(collective_id=0, has_side_effects=True),
        name="exchange",
    )(widths, hydro, face)


def update(hydro, face, halo, radial, polar, diffusion, conserved, faces_out, s, band):
    f = pl.program_id(0)
    row = lax.axis_index("row")
    shift = (120 - 16 * f) % 128
    lane = lanes((8, 128))
    sub = sublanes((8, 128))
    left, right = lane < 8, lane >= 120

    def merged(raw0, raw1, packed):
        p = pltpu.roll(packed, shift, 1)
        return jnp.where(left, p, raw0), jnp.where(right, p, raw1)

    def put(r, at, raw, packed):
        a, b = merged(raw[:, 0:128], raw[:, 128:256], packed)
        s[r, at:at + 8, 0:128] = a
        s[r, at:at + 8, 128:256] = b

    def edge_row(i):
        r = ROWS + 2 + (i - 2) if i >= 2 else i
        for j in (0, 8):
            put(r, j, radial[0, i, j:j + 8, :], polar[ROWS + i, j:j + 8, :])

    def clear_row(i):
        r = ROWS + 2 + (i - 2) if i >= 2 else i
        s[r] = jnp.zeros((CELLS + 8, THETA), F32)

    @pl.when(f == 0)
    def _():
        i0 = lax.broadcasted_iota(jnp.int32, (THETA, THETA), 0)
        i1 = lax.broadcasted_iota(jnp.int32, (THETA, THETA), 1)
        apart = jnp.abs(i0 - i1)
        band[...] = jnp.where(apart == 1, 16.0, jnp.where(apart == 2, -1.0, 0.0)).astype(jnp.bfloat16)

    @pl.when(row > 0)
    def _():
        edge_row(0)
        edge_row(1)

    @pl.when(row == 0)
    def _():
        clear_row(0)
        clear_row(1)

    @pl.when(row < NROW - 1)
    def _():
        edge_row(2)
        edge_row(3)

    @pl.when(row == NROW - 1)
    def _():
        clear_row(2)
        clear_row(3)

    def fill(ref):
        def step(r, carry):
            for j in (0, 8):
                put(r + 2, j, ref[0, r, j:j + 8, :], polar[r, j:j + 8, :])
            put(r + 2, 16, halo[0, r], polar[r, 16:24, :])
            return carry
        lax.fori_loop(0, ROWS, step, 0, unroll=4)

    def around(t0, t1, h, k):
        if k > 0:
            edge = sub >= 8 - k
            a, b, c = (pltpu.roll(t, 8 - k, 0) for t in (t0, t1, h))
            return jnp.where(edge, b, a), jnp.where(edge, c, b)
        edge = sub < -k
        a, b, c = (pltpu.roll(t, -k, 0) for t in (t0, t1, h))
        return jnp.where(edge, c, a), jnp.where(edge, a, b)

    @pl.when(f < NV)
    def _():
        fill(hydro)
        diff = diffusion[pl.ds(f, 1), :] * (1.0 / 12.0)
        batch = 4

        def step(block, carry):
            r0 = block * batch
            centre = jnp.concatenate([s[r0 + i + 2, 0:CELLS, :] for i in range(batch)], 0)
            high = centre.astype(jnp.bfloat16)
            rest = (centre - high.astype(F32)).astype(jnp.bfloat16)
            theta = jnp.dot(high, band[...], preferred_element_type=F32)
            theta = theta + jnp.dot(rest, band[...], preferred_element_type=F32)
            for i in range(batch):
                r = r0 + i + 2
                for half in range(2):
                    ln = slice(128 * half, 128 * half + 128)
                    t = [s[r, 8 * j:8 * j + 8, ln] for j in range(3)]
                    n1, n2 = around(*t, 1), around(*t, 2)
                    p1, p2 = around(*t, -1), around(*t, -2)
                    for j in range(2):
                        at = slice(8 * j, 8 * j + 8)
                        near = (n1[j] + p1[j]) + (s[r - 1, at, ln] + s[r + 1, at, ln])
                        far = (n2[j] + p2[j]) + (s[r - 2, at, ln] + s[r + 2, at, ln])
                        change = 16.0 * near - far - 90.0 * t[j]
                        change = change + theta[16 * i + 8 * j:16 * i + 8 * j + 8, ln]
                        conserved[0, r0 + i, at, ln] = t[j] + diff[:, ln] * change
            return carry

        lax.fori_loop(0, ROWS // batch, step, 0)

    @pl.when(f >= NV)
    def _():
        fill(face)

        def copy(r, carry):
            faces_out[0, r] = s[r + 2, 0:CELLS, :]
            return carry
        lax.fori_loop(0, ROWS, copy, 0, unroll=4)

    @pl.when(f == NV)
    def _():
        def step(r, carry):
            conserved[0, r] = 0.5 * (s[r + 2, 0:CELLS, :] + s[r + 3, 0:CELLS, :])
            return carry
        lax.fori_loop(0, ROWS, step, 0, unroll=4)

    @pl.when(f == NV + 1)
    def _():
        def step(r, carry):
            for j in (0, 8):
                a, b = s[r + 2, j:j + 8, 0:128], s[r + 2, j:j + 8, 128:256]
                ra, rb = pltpu.roll(a, 127, 1), pltpu.roll(b, 127, 1)
                conserved[0, r, j:j + 8, 0:128] = 0.5 * (a + jnp.where(lane == 127, rb, ra))
                conserved[0, r, j:j + 8, 128:256] = 0.5 * (b + jnp.where(lane == 127, 0.0, rb))
            return carry
        lax.fori_loop(0, ROWS, step, 0, unroll=4)

    @pl.when(f == NV + 2)
    def _():
        def step(r, carry):
            for half in range(2):
                ln = slice(128 * half, 128 * half + 128)
                t = [s[r + 2, 8 * j:8 * j + 8, ln] for j in range(3)]
                n1 = around(*t, 1)
                for j in range(2):
                    conserved[0, r, 8 * j:8 * j + 8, ln] = 0.5 * (t[j] + n1[j])
            return carry
        lax.fori_loop(0, ROWS, step, 0, unroll=4)


def run_update(hydro, face, halo, radial, polar, diffusion):
    def hyd(f):
        return (jnp.minimum(f, NV - 1), 0, 0, 0)

    def fac(f):
        return (jnp.maximum(f - NV, 0), 0, 0, 0)

    def six(f):
        return (jnp.where(f == NV + 2, NV, jnp.minimum(f, NV)), 0, 0, 0)

    return pl.pallas_call(
        update,
        grid=(FIELDS,),
        out_shape=(
            jax.ShapeDtypeStruct((FIELDS, ROWS, CELLS, THETA), F32),
            jax.ShapeDtypeStruct((NF, ROWS, CELLS, THETA), F32),
        ),
        in_specs=[
            pl.BlockSpec((1, ROWS, CELLS, THETA), hyd),
            pl.BlockSpec((1, ROWS, CELLS, THETA), fac),
            pl.BlockSpec((1, ROWS, 8, THETA), six),
            pl.BlockSpec((1, 4, CELLS, THETA), six),
            pl.BlockSpec((ROWS + 4, CELLS + 8, 128), lambda f: (0, 0, 0)),
            pl.BlockSpec((NV, THETA), lambda f: (0, 0)),
        ],
        out_specs=(
            pl.BlockSpec((1, ROWS, CELLS, THETA), lambda f: (f, 0, 0, 0)),
            pl.BlockSpec((1, ROWS, CELLS, THETA), fac),
        ),
        scratch_shapes=[
            pltpu.VMEM((ROWS + 4, CELLS + 8, THETA), F32),
            pltpu.VMEM((THETA, THETA), jnp.bfloat16),
        ],
        name="update",
    )(hydro, face, halo, radial, polar, diffusion)


def body(hydro, face, widths, diffusion):
    halo, radial, polar = run_exchange(widths, hydro, face)
    return run_update(hydro, face, halo, radial, polar, diffusion)


def solution(mesh):
    spec = P(None, "row", "phi", None)
    return jax.shard_map(
        body, mesh=mesh, in_specs=(spec, spec, P(), P()), out_specs=(spec, spec), check_vma=False
    )
```

```python
import jax
import jax.numpy as jnp
from jax import lax
from jax.experimental import pallas as pl
from jax.experimental.pallas import tpu as pltpu
from jax.sharding import PartitionSpec as P

F32 = jnp.float32
MESH = pl.DeviceIdType.MESH
NV, NF, FIELDS = 5, 3, 8
ROWS, CELLS, THETA = 32, 16, 256
NZ, NG, NROW = 8, 8, 4
EARLY = 2
FAR_FIRST = (4, 3, 5, 2, 6, 1, 7)


def lanes(shape):
    return lax.broadcasted_iota(jnp.int32, shape, len(shape) - 1)


def sublanes(shape):
    return lax.broadcasted_iota(jnp.int32, shape, len(shape) - 2)


def exchange(
    widths, hydro, face, halo, radial, polar,
    hv, fv, la, zsum, gsum, edge, first, last, first_in, last_in, la_in,
    load_sem, q_send, q_recv, qn_send, qn_recv, qp_send, qp_recv,
    la_send, la_recv, e_send, e_recv, g_send, g_recv,
    p_send, p_recv, r_send, r_recv,
):
    row, phi = lax.axis_index("row"), lax.axis_index("phi")
    z, g = phi % NZ, phi // NZ
    nphi = NZ * NG
    after, before = (phi + 1) % nphi, (phi + nphi - 1) % nphi
    has_prev, has_next = row > 0, row < NROW - 1

    def peer(d):
        return g * NZ + (z + d) % NZ

    def group(d):
        return ((g + d) % NG) * NZ + z

    loads = [pltpu.make_async_copy(hydro.at[i], hv.at[i], load_sem.at[i]) for i in range(NV)]
    loads += [pltpu.make_async_copy(face.at[i], fv.at[i], load_sem.at[NV + i]) for i in range(NF)]
    for copy in loads:
        copy.start()

    zsum[:, ROWS:, :] = jnp.zeros((NZ, 8, 128), F32)
    barrier = pltpu.get_barrier_semaphore()

    def hello(r, p):
        pl.semaphore_signal(barrier, inc=1, device_id=(r, p), device_id_type=MESH)

    for d in range(1, NZ):
        hello(row, peer(d))
        hello(row, group(d))

    @pl.when(has_prev)
    def _():
        for d in range(NZ):
            hello(row - 1, peer(d))

    @pl.when(has_next)
    def _():
        for d in range(NZ):
            hello(row + 1, peer(d))

    @pl.when(z == 0)
    def _():
        hello(row, before)

    @pl.when(z == NZ - 1)
    def _():
        hello(row, after)

    lane = lanes((8, 128))
    sub = sublanes((8, 128))
    width = jnp.zeros((8, 128), jnp.int32)
    for c in range(16):
        width = jnp.where(lane % 16 == c, widths[(c + 8) % 16], width)
    low = lane < 64

    for copy in loads:
        copy.wait()

    def pack(block, carry):
        q8 = jnp.zeros((8, 128), F32)
        f8 = jnp.zeros((8, 128), F32)
        l8 = jnp.zeros((8, 128), F32)
        for i in range(8):
            r = block * 8 + i
            parts = []
            for j in range(2):
                packed = None
                for f in range(FIELDS):
                    ref, k = (hv, f) if f < NV else (fv, f - NV)
                    t0 = ref[k, r, 8 * j:8 * j + 8, 0:128]
                    t1 = ref[k, r, 8 * j:8 * j + 8, 128:256]
                    t = pltpu.roll(jnp.where(low, t0, t1), (8 + 16 * f) % 128, 1)
                    packed = t if packed is None else jnp.where(lane // 16 == f, t, packed)
                parts.append(packed)
            sums, local = [], []
            for p in parts:
                s2 = p + jnp.where(sub % 2 == 0, pltpu.roll(p, 7, 0), pltpu.roll(p, 1, 0))
                s4 = s2 + jnp.where(sub % 4 < 2, pltpu.roll(s2, 6, 0), pltpu.roll(s2, 2, 0))
                s8 = s4 + pltpu.roll(s4, 4, 0)
                sums.append(s8)
                local.append((s2, s4, s8))
            s16 = sums[0] + sums[1]
            for j, (s2, s4, s8) in enumerate(local):
                mean = jnp.where(width == 2, s2 * 0.5, s16 * 0.0625)
                mean = jnp.where(width == 4, s4 * 0.25, mean)
                mean = jnp.where(width == 8, s8 * 0.125, mean)
                la[r, 8 * j:8 * j + 8, :] = mean
                local[j] = mean
            q8 = jnp.where(sub == i, s16, q8)
            f8 = jnp.where(sub == i, pltpu.roll(local[0], i, 0) if i else local[0], f8)
            l8 = jnp.where(sub == i, pltpu.roll(local[1], (i + 1) % 8, 0) if i < 7 else local[1], l8)
        at = pl.ds(pl.multiple_of(block * 8, 8), 8)
        zsum[z, at, :] = q8
        first[at, :] = f8
        last[at, :] = l8
        return carry

    lax.fori_loop(0, ROWS // 8, pack, 0)

    hellos = 2 * (NZ - 1) + NZ * (has_prev.astype(jnp.int32) + has_next.astype(jnp.int32))
    hellos += (z == 0).astype(jnp.int32) + (z == NZ - 1).astype(jnp.int32)
    pl.semaphore_wait(barrier, hellos)

    def remote(src, dst, ssem, rsem, r, p):
        return pltpu.make_async_remote_copy(
            src_ref=src, dst_ref=dst, send_sem=ssem, recv_sem=rsem,
            device_id=(r, p), device_id_type=MESH,
        )

    def q_copy(d):
        ref = zsum.at[z, 0:ROWS, :]
        return remote(ref, ref, q_send.at[d], q_recv.at[d], row, peer(d))

    def q_down(d):
        return remote(
            zsum.at[z, 0:2, :], zsum.at[z, ROWS + 2:ROWS + 4, :],
            qn_send.at[d], qn_recv.at[d], row - 1, peer(d),
        )

    def q_up(d):
        return remote(
            zsum.at[z, ROWS - 2:ROWS, :], zsum.at[z, ROWS:ROWS + 2, :],
            qp_send.at[d], qp_recv.at[d], row + 1, peer(d),
        )

    for d in FAR_FIRST:
        q_copy(d).start()

    @pl.when(has_prev)
    def _():
        for d in FAR_FIRST + (0,):
            q_down(d).start()

    @pl.when(has_next)
    def _():
        for d in FAR_FIRST + (0,):
            q_up(d).start()

    edge_first = remote(first, first_in, la_send.at[0], la_recv.at[0], row, before)
    edge_last = remote(last, last_in, la_send.at[1], la_recv.at[1], row, after)
    edge_first.start()
    edge_last.start()
    la_down = remote(la.at[0:2], la_in.at[2:4], la_send.at[2], la_recv.at[2], row - 1, phi)
    la_up = remote(la.at[ROWS - 2:ROWS], la_in.at[0:2], la_send.at[3], la_recv.at[3], row + 1, phi)

    down = [remote(hv.at[:, 0:2], radial.at[0:NV, 2:4], r_send.at[0], r_recv.at[0], row - 1, phi)]
    down += [remote(fv.at[0, 0:1], radial.at[NV, 2:3], r_send.at[1], r_recv.at[1], row - 1, phi)]
    up = [remote(hv.at[:, ROWS - 2:ROWS], radial.at[0:NV, 0:2], r_send.at[2], r_recv.at[2], row + 1, phi)]

    @pl.when(has_prev)
    def _():
        la_down.start()
        for copy in down:
            copy.start()

    @pl.when(has_next)
    def _():
        la_up.start()
        for copy in up:
            copy.start()

    bulk = []
    for i in range(NV):
        bulk.append(remote(
            hv.at[i, :, CELLS - 2:CELLS, :], halo.at[i, :, 6:8, :],
            p_send.at[2 * i], p_recv.at[2 * i], row, after,
        ))
        bulk.append(remote(
            hv.at[i, :, 0:2, :], halo.at[i, :, 0:2, :],
            p_send.at[2 * i + 1], p_recv.at[2 * i + 1], row, before,
        ))
    bulk.append(remote(
        fv.at[2, :, 0:1, :], halo.at[NV, :, 0:1, :],
        p_send.at[2 * NV], p_recv.at[2 * NV], row, before,
    ))
    for copy in bulk[:2 * EARLY]:
        copy.start()

    for d in FAR_FIRST:
        q_copy(d).wait_recv()

    @pl.when(has_prev)
    def _():
        for d in FAR_FIRST + (0,):
            q_up(d).wait_recv()

    @pl.when(has_next)
    def _():
        for d in FAR_FIRST + (0,):
            q_down(d).wait_recv()

    def z_sums(at):
        pair, quad = (at // 2) * 2, (at // 4) * 4
        s32 = zsum[pair] + zsum[pair + 1]
        s64 = (zsum[quad] + zsum[quad + 1]) + (zsum[quad + 2] + zsum[quad + 3])
        return s32, s64

    tall = (ROWS + 8, 128)
    width = jnp.broadcast_to(width[0:1], tall)
    total = zsum[0]
    for i in range(1, NZ):
        total = total + zsum[i]
    gsum[g] = total

    def g_copy(d):
        return remote(gsum.at[g], gsum.at[g], g_send.at[d], g_recv.at[d], row, group(d))

    for d in (5, 3, 7, 1, 6, 2, 4):
        g_copy(d).start()

    s32, s64 = z_sums(z)
    small = jnp.where(width == 32, s32 * (1 / 32), s64 * (1 / 64))
    s32p, s64p = z_sums((z + NZ - 1) % NZ)
    s32n, s64n = z_sums((z + 1) % NZ)
    edge[0] = jnp.where(width == 32, s32p * (1 / 32), s64p * (1 / 64))[:ROWS]
    edge[1] = jnp.where(width == 32, s32n * (1 / 32), s64n * (1 / 64))[:ROWS]
    edge_up = remote(edge.at[0], edge.at[2], e_send.at[0], e_recv.at[0], row, group(1))
    edge_down = remote(edge.at[1], edge.at[3], e_send.at[1], e_recv.at[1], row, group(NG - 1))

    edge_up.start()
    edge_down.start()

    for copy in bulk[2 * EARLY:]:
        copy.start()

    for d in (5, 3, 7, 1, 6, 2, 4):
        g_copy(d).wait_recv()
    edge_up.wait_recv()
    edge_down.wait_recv()
    edge_first.wait_recv()
    edge_last.wait_recv()

    def g_means(at, small):
        pair, quad = (at // 2) * 2, (at // 4) * 4
        mean = jnp.where(width == 128, gsum[at] * (1 / 128), small)
        mean = jnp.where(width == 256, (gsum[pair] + gsum[pair + 1]) * (1 / 256), mean)
        four = (gsum[quad] + gsum[quad + 1]) + (gsum[quad + 2] + gsum[quad + 3])
        mean = jnp.where(width == 512, four * (1 / 512), mean)
        whole = gsum[0]
        for i in range(1, NG):
            whole = whole + gsum[i]
        return jnp.where(width == 1024, whole * (1 / 1024), mean)

    mean = g_means(g, small)
    gp = jnp.where(z == 0, (g + NG - 1) % NG, g)
    gn = jnp.where(z == NZ - 1, (g + 1) % NG, g)
    pad = jnp.zeros((8, 128), F32)
    ep = jnp.concatenate([jnp.where(z == 0, edge[2], edge[0]), pad])
    en = jnp.concatenate([jnp.where(z == NZ - 1, edge[3], edge[1]), pad])
    mean_p = jnp.where(width <= 16, jnp.concatenate([last_in[...], pad]), g_means(gp, ep))
    mean_n = jnp.where(width <= 16, jnp.concatenate([first_in[...], pad]), g_means(gn, en))
    narrow = jnp.broadcast_to(width[0:1], (CELLS, 128)) <= 16
    for r in range(ROWS):
        polar[r, 0:CELLS, :] = jnp.where(narrow, la[r], mean[r:r + 1])
        polar[r, CELLS:, :] = jnp.where(sub < 4, mean_n[r:r + 1], mean_p[r:r + 1])

    @pl.when(has_prev)
    def _():
        la_up.wait_recv()

    @pl.when(has_next)
    def _():
        la_down.wait_recv()

    for i in range(4):
        r = ROWS + i
        polar[r, 0:CELLS, :] = jnp.where(narrow, la_in[i], mean[r:r + 1])
        polar[r, CELLS:, :] = jnp.zeros((8, 128), F32)

    for copy in bulk:
        copy.wait_recv()

    @pl.when(has_prev)
    def _():
        for copy in up:
            copy.wait_recv()

    @pl.when(has_next)
    def _():
        for copy in down:
            copy.wait_recv()

    for d in FAR_FIRST:
        q_copy(d).wait_send()
        g_copy(d).wait_send()
    for copy in bulk + [edge_up, edge_down, edge_first, edge_last]:
        copy.wait_send()

    @pl.when(has_prev)
    def _():
        la_down.wait_send()
        for copy in down:
            copy.wait_send()
        for d in range(NZ):
            q_down(d).wait_send()

    @pl.when(has_next)
    def _():
        la_up.wait_send()
        for copy in up:
            copy.wait_send()
        for d in range(NZ):
            q_up(d).wait_send()


def run_exchange(widths, hydro, face):
    dma = pltpu.SemaphoreType.DMA
    return pl.pallas_call(
        exchange,
        out_shape=(
            jax.ShapeDtypeStruct((NV + 1, ROWS, 8, THETA), F32),
            jax.ShapeDtypeStruct((NV + 1, 4, CELLS, THETA), F32),
            jax.ShapeDtypeStruct((ROWS + 4, CELLS + 8, 128), F32),
        ),
        in_specs=[
            pl.BlockSpec(memory_space=pltpu.SMEM),
            pl.BlockSpec(memory_space=pltpu.HBM),
            pl.BlockSpec(memory_space=pltpu.HBM),
        ],
        out_specs=(
            pl.BlockSpec(memory_space=pltpu.VMEM),
            pl.BlockSpec(memory_space=pltpu.VMEM),
            pl.BlockSpec(memory_space=pltpu.VMEM),
        ),
        scratch_shapes=[
            pltpu.VMEM((NV, ROWS, CELLS, THETA), F32),
            pltpu.VMEM((NF, ROWS, CELLS, THETA), F32),
            pltpu.VMEM((ROWS, CELLS, 128), F32),
            pltpu.VMEM((NZ, ROWS + 8, 128), F32),
            pltpu.VMEM((NG, ROWS + 8, 128), F32),
            pltpu.VMEM((4, ROWS, 128), F32),
            pltpu.VMEM((ROWS, 128), F32),
            pltpu.VMEM((ROWS, 128), F32),
            pltpu.VMEM((ROWS, 128), F32),
            pltpu.VMEM((ROWS, 128), F32),
            pltpu.VMEM((4, CELLS, 128), F32),
            dma((FIELDS,)),
            dma((NZ,)), dma((NZ,)), dma((NZ,)), dma((NZ,)), dma((NZ,)), dma((NZ,)),
            dma((4,)), dma((4,)), dma((2,)), dma((2,)), dma((NG,)), dma((NG,)),
            dma((2 * NV + 1,)), dma((2 * NV + 1,)), dma((3,)), dma((3,)),
        ],
        compiler_params=pltpu.CompilerParams(
            collective_id=0, has_side_effects=True, vmem_limit_bytes=51 << 20
        ),
        name="exchange",
    )(widths, hydro, face)


def update(
    hydro, face, halo, radial, polar, diffusion, conserved, faces_out,
    s, co, fo, store_sem,
):
    row = lax.axis_index("row")
    lane = lanes((8, 128))
    sub = sublanes((8, 128))
    left, right = lane < 8, lane >= 120
    i0 = lax.broadcasted_iota(jnp.int32, (THETA, THETA), 0)
    i1 = lax.broadcasted_iota(jnp.int32, (THETA, THETA), 1)
    apart = jnp.abs(i0 - i1)
    band = jnp.where(apart == 0, -90.0, jnp.where(apart == 1, 16.0, jnp.where(apart == 2, -1.0, 0.0)))
    band = band.astype(jnp.bfloat16)

    def around(t0, t1, h, k):
        if k > 0:
            edge = sub >= 8 - k
            a, b, c = (pltpu.roll(t, 8 - k, 0) for t in (t0, t1, h))
            return jnp.where(edge, b, a), jnp.where(edge, c, b)
        edge = sub < -k
        a, b, c = (pltpu.roll(t, -k, 0) for t in (t0, t1, h))
        return jnp.where(edge, c, a), jnp.where(edge, a, b)

    def fill(f, ref, k):
        shift = (120 - 16 * f) % 128

        def put(r, at, raw, packed):
            p = pltpu.roll(packed, shift, 1)
            s[r, at:at + 8, 0:128] = jnp.where(left, p, raw[:, 0:128])
            s[r, at:at + 8, 128:256] = jnp.where(right, p, raw[:, 128:256])

        def edge_row(i):
            r = ROWS + i if i >= 2 else i
            for j in (0, 8):
                put(r, j, radial[min(f, NV), i, j:j + 8, :], polar[ROWS + i, j:j + 8, :])

        if f <= NV:
            for side, wide in ((row > 0, (0, 1)), (row < NROW - 1, (2, 3))):
                @pl.when(side)
                def _():
                    for i in wide:
                        edge_row(i)

                @pl.when(jnp.logical_not(side))
                def _():
                    for i in wide:
                        s[ROWS + i if i >= 2 else i] = jnp.zeros((CELLS + 8, THETA), F32)

        def step(r, carry):
            for j in (0, 8):
                put(r + 2, j, ref[k, r, j:j + 8, :], polar[r, j:j + 8, :])
            if f < NV or f == NV + 2:
                put(r + 2, 16, halo[min(f, NV), r], polar[r, 16:24, :])
            return carry
        lax.fori_loop(0, ROWS, step, 0, unroll=8)

    for f in range(NV):
        fill(f, hydro, f)
        diff = diffusion[f:f + 1, :] * (1.0 / 12.0)
        batch = 8

        def step(block, carry):
            r0 = block * batch
            centre = jnp.concatenate([s[r0 + i + 2, 0:CELLS, :] for i in range(batch)], 0)
            high = centre.astype(jnp.bfloat16)
            rest = (centre - high.astype(F32)).astype(jnp.bfloat16)
            theta = jnp.dot(high, band, preferred_element_type=F32)
            theta = theta + jnp.dot(rest, band, preferred_element_type=F32)
            for i in range(batch):
                r = r0 + i + 2
                for half in range(2):
                    ln = slice(128 * half, 128 * half + 128)
                    t = [s[r, 8 * j:8 * j + 8, ln] for j in range(3)]
                    n1, n2 = around(*t, 1), around(*t, 2)
                    p1, p2 = around(*t, -1), around(*t, -2)
                    for j in range(2):
                        at = slice(8 * j, 8 * j + 8)
                        near = (n1[j] + p1[j]) + (s[r - 1, at, ln] + s[r + 1, at, ln])
                        far = (n2[j] + p2[j]) + (s[r - 2, at, ln] + s[r + 2, at, ln])
                        change = 16.0 * near - far
                        change = change + theta[16 * i + 8 * j:16 * i + 8 * j + 8, ln]
                        co[f, r0 + i, at, ln] = t[j] + diff[:, ln] * change
            return carry

        lax.fori_loop(0, ROWS // batch, step, 0)
        pltpu.make_async_copy(co.at[f], conserved.at[f], store_sem.at[f]).start()

    for k in range(NF):
        f = NV + k
        fill(f, face, k)

        def step(r, carry):
            fo[k, r] = s[r + 2, 0:CELLS, :]
            if k == 0:
                co[f, r] = 0.5 * (s[r + 2, 0:CELLS, :] + s[r + 3, 0:CELLS, :])
            elif k == 1:
                for j in (0, 8):
                    a, b = s[r + 2, j:j + 8, 0:128], s[r + 2, j:j + 8, 128:256]
                    ra, rb = pltpu.roll(a, 127, 1), pltpu.roll(b, 127, 1)
                    co[f, r, j:j + 8, 0:128] = 0.5 * (a + jnp.where(lane == 127, rb, ra))
                    co[f, r, j:j + 8, 128:256] = 0.5 * (b + jnp.where(lane == 127, 0.0, rb))
            else:
                for half in range(2):
                    ln = slice(128 * half, 128 * half + 128)
                    t = [s[r + 2, 8 * j:8 * j + 8, ln] for j in range(3)]
                    n1 = around(*t, 1)
                    for j in range(2):
                        co[f, r, 8 * j:8 * j + 8, ln] = 0.5 * (t[j] + n1[j])
            return carry
        lax.fori_loop(0, ROWS, step, 0, unroll=8)
        pltpu.make_async_copy(co.at[f], conserved.at[f], store_sem.at[f]).start()
        pltpu.make_async_copy(fo.at[k], faces_out.at[k], store_sem.at[FIELDS + k]).start()

    for f in range(FIELDS):
        pltpu.make_async_copy(co.at[f], conserved.at[f], store_sem.at[f]).wait()
    for k in range(NF):
        pltpu.make_async_copy(fo.at[k], faces_out.at[k], store_sem.at[FIELDS + k]).wait()


def run_update(hydro, face, halo, radial, polar, diffusion):
    return pl.pallas_call(
        update,
        out_shape=(
            jax.ShapeDtypeStruct((FIELDS, ROWS, CELLS, THETA), F32),
            jax.ShapeDtypeStruct((NF, ROWS, CELLS, THETA), F32),
        ),
        in_specs=[pl.BlockSpec(memory_space=pltpu.VMEM)] * 6,
        out_specs=(pl.BlockSpec(memory_space=pltpu.HBM), pl.BlockSpec(memory_space=pltpu.HBM)),
        scratch_shapes=[
            pltpu.VMEM((ROWS + 4, CELLS + 8, THETA), F32),
            pltpu.VMEM((FIELDS, ROWS, CELLS, THETA), F32),
            pltpu.VMEM((NF, ROWS, CELLS, THETA), F32),
            pltpu.SemaphoreType.DMA((FIELDS + NF,)),
        ],
        compiler_params=pltpu.CompilerParams(vmem_limit_bytes=24 << 20),
        name="update",
    )(hydro, face, halo, radial, polar, diffusion)


def body(hydro, face, widths, diffusion):
    halo, radial, polar = run_exchange(widths, hydro, face)
    return run_update(hydro, face, halo, radial, polar, diffusion)


def solution(mesh):
    spec = P(None, "row", "phi", None)
    return jax.shard_map(
        body, mesh=mesh, in_specs=(spec, spec, P(), P()), out_specs=(spec, spec), check_vma=False
    )
```

```python
import jax
import jax.numpy as jnp
from jax import lax
from jax.experimental import pallas as pl
from jax.experimental.pallas import tpu as pltpu
from jax.sharding import PartitionSpec as P

F32 = jnp.float32
MESH = pl.DeviceIdType.MESH
NV, NF, FIELDS = 5, 3, 8
ROWS, CELLS, THETA = 32, 16, 256
NZ, NG, NROW = 8, 8, 4
EARLY = 5
BATCH = 8
FAR_FIRST = (4, 3, 5, 2, 6, 1, 7)


def lanes(shape):
    return lax.broadcasted_iota(jnp.int32, shape, len(shape) - 1)


def sublanes(shape):
    return lax.broadcasted_iota(jnp.int32, shape, len(shape) - 2)


def around(t0, t1, h, k, sub):
    if k > 0:
        edge = sub >= 8 - k
        a, b, c = (None if t is None else pltpu.roll(t, 8 - k, 0) for t in (t0, t1, h))
        return jnp.where(edge, b, a), jnp.where(edge, 0.0 if c is None else c, b)
    edge = sub < -k
    a, b, c = (None if t is None else pltpu.roll(t, -k, 0) for t in (t0, t1, h))
    return jnp.where(edge, 0.0 if c is None else c, a), jnp.where(edge, a, b)


def exchange(
    widths_hbm, hydro, face, diffusion_hbm, pre, even, odd, packed_out,
    hv, fv, halo, radial, la, pp, zsum, gsum, edge, first, last, first_in, last_in, la_in,
    dd, mm, widths, diffusion, small_sem,
    load_sem, q_send, q_recv, qn_send, qn_recv, qp_send, qp_recv,
    la_send, la_recv, e_send, e_recv, g_send, g_recv,
    p_send, p_recv, r_send, r_recv,
):
    row, phi = lax.axis_index("row"), lax.axis_index("phi")
    z, g = phi % NZ, phi // NZ
    nphi = NZ * NG
    after, before = (phi + 1) % nphi, (phi + nphi - 1) % nphi
    has_prev, has_next = row > 0, row < NROW - 1

    def peer(d):
        return g * NZ + (z + d) % NZ

    def group(d):
        return ((g + d) % NG) * NZ + z

    get_widths = pltpu.make_async_copy(widths_hbm, widths, small_sem.at[0])
    get_diffusion = pltpu.make_async_copy(diffusion_hbm, diffusion, small_sem.at[1])
    get_widths.start()
    loads = []
    for i in range(4):
        loads.append((
            pltpu.make_async_copy(hydro.at[:, 8 * i:8 * i + 8], hv.at[:, 8 * i + 2:8 * i + 10], load_sem.at[2 * i]),
            pltpu.make_async_copy(face.at[:, 8 * i:8 * i + 8], fv.at[:, 8 * i:8 * i + 8], load_sem.at[2 * i + 1]),
        ))
        for copy in loads[i]:
            copy.start()
    get_diffusion.start()

    zsum[:, ROWS:, :] = jnp.zeros((NZ, 8, 128), F32)
    barrier = pltpu.get_barrier_semaphore()

    def hello(r, p):
        pl.semaphore_signal(barrier, inc=1, device_id=(r, p), device_id_type=MESH)

    for d in range(1, NZ):
        hello(row, peer(d))
        hello(row, group(d))

    @pl.when(has_prev)
    def _():
        for d in range(NZ):
            hello(row - 1, peer(d))

    @pl.when(has_next)
    def _():
        for d in range(NZ):
            hello(row + 1, peer(d))

    @pl.when(z == 0)
    def _():
        hello(row, before)

    @pl.when(z == NZ - 1)
    def _():
        hello(row, after)

    for i in range(NV):
        for r in (0, 1, ROWS + 2, ROWS + 3):
            hv[i, r] = jnp.zeros((CELLS, THETA), F32)

    lane = lanes((8, 128))
    sub = sublanes((8, 128))
    low = lane < 64
    get_widths.wait()
    width = jnp.zeros((8, 128), jnp.int32)
    for c in range(16):
        width = jnp.where(lane % 16 == c, widths[(c + 8) % 16], width)

    def pack(block, base):
        q8 = jnp.zeros((8, 128), F32)
        f8 = jnp.zeros((8, 128), F32)
        l8 = jnp.zeros((8, 128), F32)
        for i in range(8):
            r = block * 8 + i
            sums, local = [], []
            for j in range(2):
                p = None
                for f in range(FIELDS):
                    ref, k, at = (hv, f, r + 2) if f < NV else (fv, f - NV, r)
                    t0 = ref[k, at, 8 * j:8 * j + 8, 0:128]
                    t1 = ref[k, at, 8 * j:8 * j + 8, 128:256]
                    t = jnp.where(low, t0, t1)
                    shift = (8 + 16 * f) % 128
                    t = pltpu.roll(t, shift, 1)
                    p = t if p is None else jnp.where(lane // 16 == f, t, p)
                pp[r, 8 * j:8 * j + 8, :] = p
                s2 = p + jnp.where(sub % 2 == 0, pltpu.roll(p, 7, 0), pltpu.roll(p, 1, 0))
                s4 = s2 + jnp.where(sub % 4 < 2, pltpu.roll(s2, 6, 0), pltpu.roll(s2, 2, 0))
                s8 = s4 + pltpu.roll(s4, 4, 0)
                sums.append(s8)
                local.append((s2, s4, s8))
            s16 = sums[0] + sums[1]
            for j, (s2, s4, s8) in enumerate(local):
                mean = jnp.where(width == 2, s2 * 0.5, s16 * 0.0625)
                mean = jnp.where(width == 4, s4 * 0.25, mean)
                mean = jnp.where(width == 8, s8 * 0.125, mean)
                la[r, 8 * j:8 * j + 8, :] = mean
                local[j] = mean
            q8 = jnp.where(sub == i, s16, q8)
            f8 = jnp.where(sub == i, pltpu.roll(local[0], i, 0) if i else local[0], f8)
            l8 = jnp.where(sub == i, pltpu.roll(local[1], (i + 1) % 8, 0) if i < 7 else local[1], l8)
        at = pl.ds(pl.multiple_of(block * 8, 8), 8)
        zsum[z, at, :] = q8
        first[at, :] = f8
        last[at, :] = l8
        return base

    for i in range(4):
        for copy in loads[i]:
            copy.wait()
        pack(i, 0)

    hellos = 2 * (NZ - 1) + NZ * (has_prev.astype(jnp.int32) + has_next.astype(jnp.int32))
    hellos += (z == 0).astype(jnp.int32) + (z == NZ - 1).astype(jnp.int32)
    pl.semaphore_wait(barrier, hellos)

    def remote(src, dst, ssem, rsem, r, p):
        return pltpu.make_async_remote_copy(
            src_ref=src, dst_ref=dst, send_sem=ssem, recv_sem=rsem,
            device_id=(r, p), device_id_type=MESH,
        )

    def q_copy(d):
        ref = zsum.at[z, 0:ROWS, :]
        return remote(ref, ref, q_send.at[d], q_recv.at[d], row, peer(d))

    def q_down(d):
        return remote(
            zsum.at[z, 0:2, :], zsum.at[z, ROWS + 2:ROWS + 4, :],
            qn_send.at[d], qn_recv.at[d], row - 1, peer(d),
        )

    def q_up(d):
        return remote(
            zsum.at[z, ROWS - 2:ROWS, :], zsum.at[z, ROWS:ROWS + 2, :],
            qp_send.at[d], qp_recv.at[d], row + 1, peer(d),
        )

    for d in FAR_FIRST:
        q_copy(d).start()

    @pl.when(has_prev)
    def _():
        for d in FAR_FIRST + (0,):
            q_down(d).start()

    @pl.when(has_next)
    def _():
        for d in FAR_FIRST + (0,):
            q_up(d).start()

    edge_first = remote(first, first_in, la_send.at[0], la_recv.at[0], row, before)
    edge_last = remote(last, last_in, la_send.at[1], la_recv.at[1], row, after)
    edge_first.start()
    edge_last.start()
    la_down = remote(la.at[0:2], la_in.at[2:4], la_send.at[2], la_recv.at[2], row - 1, phi)
    la_up = remote(la.at[ROWS - 2:ROWS], la_in.at[0:2], la_send.at[3], la_recv.at[3], row + 1, phi)

    down = [remote(hv.at[:, 2:4], radial.at[0:NV, 2:4], r_send.at[0], r_recv.at[0], row - 1, phi)]
    down += [remote(fv.at[0, 0:1], radial.at[NV, 2:3], r_send.at[1], r_recv.at[1], row - 1, phi)]
    up = [remote(hv.at[:, ROWS:ROWS + 2], radial.at[0:NV, 0:2], r_send.at[2], r_recv.at[2], row + 1, phi)]

    @pl.when(has_prev)
    def _():
        la_down.start()
        for copy in down:
            copy.start()

    @pl.when(has_next)
    def _():
        la_up.start()
        for copy in up:
            copy.start()

    bulk = []
    for i in range(NV):
        bulk.append(remote(
            hv.at[i, 2:ROWS + 2, CELLS - 2:CELLS, :], halo.at[i, :, 6:8, :],
            p_send.at[2 * i], p_recv.at[2 * i], row, after,
        ))
        bulk.append(remote(
            hv.at[i, 2:ROWS + 2, 0:2, :], halo.at[i, :, 0:2, :],
            p_send.at[2 * i + 1], p_recv.at[2 * i + 1], row, before,
        ))
    bulk.append(remote(
        fv.at[2, :, 0:1, :], halo.at[NV, :, 0:1, :],
        p_send.at[2 * NV], p_recv.at[2 * NV], row, before,
    ))
    for copy in bulk[:2 * EARLY]:
        copy.start()

    get_diffusion.wait()
    i0 = lax.broadcasted_iota(jnp.int32, (THETA, THETA), 0)
    i1 = lax.broadcasted_iota(jnp.int32, (THETA, THETA), 1)
    apart = jnp.abs(i0 - i1)
    band = jnp.where(apart == 0, -90.0, jnp.where(apart == 1, 16.0, jnp.where(apart == 2, -1.0, 0.0)))
    band = band.astype(jnp.bfloat16)

    def raw_field(f):
        diff = diffusion[f:f + 1, :] * (1.0 / 12.0)

        def step(block, carry):
            r0 = block * BATCH
            centre = jnp.concatenate([hv[f, r0 + i + 2] for i in range(BATCH)], 0)
            high = centre.astype(jnp.bfloat16)
            rest = (centre - high.astype(F32)).astype(jnp.bfloat16)
            theta = jnp.dot(high, band, preferred_element_type=F32)
            theta = theta + jnp.dot(rest, band, preferred_element_type=F32)
            for i in range(BATCH):
                r = r0 + i + 2
                for half in range(2):
                    ln = slice(128 * half, 128 * half + 128)
                    t = [hv[f, r, 8 * j:8 * j + 8, ln] for j in range(2)] + [None]
                    n1, n2 = around(*t, 1, sub), around(*t, 2, sub)
                    p1, p2 = around(*t, -1, sub), around(*t, -2, sub)
                    for j in range(2):
                        at = slice(8 * j, 8 * j + 8)
                        near = (n1[j] + p1[j]) + (hv[f, r - 1, at, ln] + hv[f, r + 1, at, ln])
                        far = (n2[j] + p2[j]) + (hv[f, r - 2, at, ln] + hv[f, r + 2, at, ln])
                        change = 16.0 * near - far
                        change = change + theta[16 * i + 8 * j:16 * i + 8 * j + 8, ln]
                        pre[f, r0 + i, at, ln] = t[j] + diff[:, ln] * change
            return carry

        lax.fori_loop(0, ROWS // BATCH, step, 0)

    def raw_faces():
        def step(r, carry):
            for j in (0, 8):
                a, b = fv[1, r, j:j + 8, 0:128], fv[1, r, j:j + 8, 128:256]
                ra, rb = pltpu.roll(a, 127, 1), pltpu.roll(b, 127, 1)
                pre[NV + 1, r, j:j + 8, 0:128] = 0.5 * (a + jnp.where(lane == 127, rb, ra))
                pre[NV + 1, r, j:j + 8, 128:256] = 0.5 * (b + jnp.where(lane == 127, 0.0, rb))
            for half in range(2):
                ln = slice(128 * half, 128 * half + 128)
                t = [fv[2, r, 8 * j:8 * j + 8, ln] for j in range(2)]
                n1 = around(t[0], t[1], None, 1, sub)
                for j in range(2):
                    pre[NV + 2, r, 8 * j:8 * j + 8, ln] = 0.5 * (t[j] + n1[j])
            return carry
        lax.fori_loop(0, ROWS, step, 0, unroll=4)

        def mean_step(r, carry):
            pre[NV, r] = 0.5 * (fv[0, r] + fv[0, r + 1])
            return carry
        lax.fori_loop(0, ROWS - 1, mean_step, 0)
        pre[NV, ROWS - 1] = 0.5 * fv[0, ROWS - 1]

    for f in range(NV):
        raw_field(f)

    for d in FAR_FIRST:
        q_copy(d).wait_recv()

    @pl.when(has_prev)
    def _():
        for d in FAR_FIRST + (0,):
            q_up(d).wait_recv()

    @pl.when(has_next)
    def _():
        for d in FAR_FIRST + (0,):
            q_down(d).wait_recv()

    def z_sums(at):
        pair, quad = (at // 2) * 2, (at // 4) * 4
        s32 = zsum[pair] + zsum[pair + 1]
        s64 = (zsum[quad] + zsum[quad + 1]) + (zsum[quad + 2] + zsum[quad + 3])
        return s32, s64

    tall = (ROWS + 8, 128)
    wide = jnp.broadcast_to(width[0:1], tall)
    total = zsum[0]
    for i in range(1, NZ):
        total = total + zsum[i]
    gsum[g] = total

    def g_copy(d):
        return remote(gsum.at[g], gsum.at[g], g_send.at[d], g_recv.at[d], row, group(d))

    for d in (5, 3, 7, 1, 6, 2, 4):
        g_copy(d).start()

    s32p, s64p = z_sums((z + NZ - 1) % NZ)
    s32n, s64n = z_sums((z + 1) % NZ)
    edge[0] = jnp.where(wide == 32, s32p * (1 / 32), s64p * (1 / 64))[:ROWS]
    edge[1] = jnp.where(wide == 32, s32n * (1 / 32), s64n * (1 / 64))[:ROWS]
    edge_up = remote(edge.at[0], edge.at[2], e_send.at[0], e_recv.at[0], row, group(1))
    edge_down = remote(edge.at[1], edge.at[3], e_send.at[1], e_recv.at[1], row, group(NG - 1))
    edge_up.start()
    edge_down.start()

    for copy in bulk[2 * EARLY:]:
        copy.start()

    raw_faces()

    seg, m = lane // 16, lane % 16
    is_even = seg % 2 == 0
    diff_even = jnp.zeros((8, 128), F32)
    diff_odd = jnp.zeros((8, 128), F32)
    for f in range(NV):
        t = jnp.where(low, diffusion[f:f + 1, 0:128], diffusion[f:f + 1, 128:256])
        t = pltpu.roll(jnp.broadcast_to(t, (8, 128)), (8 + 16 * f) % 128, 1) * (1.0 / 12.0)
        near_f = (lane - 16 * f + 2 + 128) % 128 < 20
        if f % 2 == 0:
            diff_even = jnp.where(near_f, t, diff_even)
        else:
            diff_odd = jnp.where(near_f, t, diff_odd)
    own = jnp.where(is_even, diff_even, diff_odd)
    out = jnp.where(is_even, diff_odd, diff_even)
    fluid = seg < NV
    zero = jnp.zeros((8, 128), F32)
    c0 = jnp.where(fluid, 1.0 - 90.0 * own, 0.5)
    c1 = jnp.where(fluid, 16.0 * own, zero)
    c2 = jnp.where(fluid, -own, zero)
    c_row = jnp.where(seg == NV, 0.5, zero)
    c_cell = jnp.where(seg == NV + 2, 0.5, zero)
    k1p = jnp.where(m % 8 == 0, zero, c1)
    k1n = jnp.where(m % 8 == 7, zero, c1 + jnp.where(seg == NV + 1, 0.5, zero))
    k2p = jnp.where(m % 8 < 2, zero, c2)
    k2n = jnp.where(m % 8 > 5, zero, c2)
    from_left = (seg + 7) % 8
    from_right = (seg + 1) % 8
    left_fluid, right_fluid = from_left < NV, from_right < NV
    s1p = jnp.where(jnp.logical_and(m == 0, left_fluid), 16.0 * out, zero)
    s2p = jnp.where(jnp.logical_and(m < 2, left_fluid), -out, zero)
    s1n = jnp.where(jnp.logical_and(m == 15, right_fluid), 16.0 * out, zero)
    s1n = jnp.where(jnp.logical_and(m == 15, from_right == NV + 1), 0.5, s1n)
    s2n = jnp.where(jnp.logical_and(m > 13, right_fluid), -out, zero)

    inner = (lane >= 8, lane < 120)

    @pl.when(has_prev)
    def _():
        for copy in up:
            copy.wait_recv()
        for f in range(NV):
            for half in range(2):
                ln = slice(128 * half, 128 * half + 128)
                diff = diffusion[f:f + 1, ln] * (1.0 / 12.0)
                for at in (slice(0, 8), slice(8, 16)):
                    b2, b1 = (jnp.where(inner[half], radial[f, i, at, ln], 0.0) for i in (0, 1))
                    pre[f, 0, at, ln] = pre[f, 0, at, ln] + diff * (16.0 * b1 - b2)
                    pre[f, 1, at, ln] = pre[f, 1, at, ln] - diff * b1

    @pl.when(has_next)
    def _():
        for copy in down:
            copy.wait_recv()
        for half in range(2):
            ln = slice(128 * half, 128 * half + 128)
            for at in (slice(0, 8), slice(8, 16)):
                for f in range(NV):
                    diff = diffusion[f:f + 1, ln] * (1.0 / 12.0)
                    b1, b2 = (jnp.where(inner[half], radial[f, i, at, ln], 0.0) for i in (2, 3))
                    e, e1 = ROWS - 1, ROWS - 2
                    pre[f, e, at, ln] = pre[f, e, at, ln] + diff * (16.0 * b1 - b2)
                    pre[f, e1, at, ln] = pre[f, e1, at, ln] - diff * b1
                b = jnp.where(inner[half], radial[NV, 2, at, ln], 0.0)
                pre[NV, ROWS - 1, at, ln] = pre[NV, ROWS - 1, at, ln] + 0.5 * b

    a1 = jnp.where(sub == 0, 16.0, zero)
    a2 = jnp.where(sub < 2, -1.0, zero)
    b1 = jnp.where(sub == 7, 16.0, zero)
    b2 = jnp.where(sub > 5, -1.0, zero)
    for f in range(NV):
        bulk[2 * f].wait_recv()
        bulk[2 * f + 1].wait_recv()
        diffs = [diffusion[f:f + 1, 128 * half:128 * half + 128] * (1.0 / 12.0) for half in range(2)]

        def step(r, carry):
            for half in range(2):
                ln = slice(128 * half, 128 * half + 128)
                h = jnp.where(inner[half], halo[f, r, :, ln], 0.0) * diffs[half]
                head = a1 * pltpu.roll(h, 1, 0) + a2 * pltpu.roll(h, 2, 0)
                tail = b1 * pltpu.roll(h, 7, 0) + b2 * pltpu.roll(h, 6, 0)
                pre[f, r, 0:8, ln] = pre[f, r, 0:8, ln] + head
                pre[f, r, 8:16, ln] = pre[f, r, 8:16, ln] + tail
            return carry
        lax.fori_loop(0, ROWS, step, 0, unroll=8)
    bulk[2 * NV].wait_recv()

    def face_step(r, carry):
        for half in range(2):
            ln = slice(128 * half, 128 * half + 128)
            h = pltpu.roll(halo[NV, r, :, ln], 7, 0)
            h = jnp.where(jnp.logical_and(inner[half], sub == 7), 0.5 * h, 0.0)
            pre[NV + 2, r, 8:16, ln] = pre[NV + 2, r, 8:16, ln] + h
        return carry
    lax.fori_loop(0, ROWS, face_step, 0, unroll=8)

    for d in (5, 3, 7, 1, 6, 2, 4):
        g_copy(d).wait_recv()
    edge_up.wait_recv()
    edge_down.wait_recv()
    edge_first.wait_recv()
    edge_last.wait_recv()

    whole = gsum[0]
    for i in range(1, NG):
        whole = whole + gsum[i]
    whole = whole * (1 / 1024)

    def g_means(at, small):
        pair, quad = (at // 2) * 2, (at // 4) * 4
        mean = jnp.where(wide == 128, gsum[at] * (1 / 128), small)
        mean = jnp.where(wide == 256, (gsum[pair] + gsum[pair + 1]) * (1 / 256), mean)
        four = (gsum[quad] + gsum[quad + 1]) + (gsum[quad + 2] + gsum[quad + 3])
        mean = jnp.where(wide == 512, four * (1 / 512), mean)
        return jnp.where(wide == 1024, whole, mean)

    s32, s64 = z_sums(z)
    mm[0] = g_means(g, jnp.where(wide == 32, s32 * (1 / 32), s64 * (1 / 64)))
    gp = jnp.where(z == 0, (g + NG - 1) % NG, g)
    gn = jnp.where(z == NZ - 1, (g + 1) % NG, g)
    pad = jnp.zeros((8, 128), F32)
    ep = jnp.concatenate([jnp.where(z == 0, edge[2], edge[0]), pad])
    en = jnp.concatenate([jnp.where(z == NZ - 1, edge[3], edge[1]), pad])
    mm[1] = jnp.where(wide <= 16, jnp.concatenate([last_in[...], pad]), g_means(gp, ep))
    mm[2] = jnp.where(wide <= 16, jnp.concatenate([first_in[...], pad]), g_means(gn, en))
    narrow = width <= 16

    def differ(r, carry):
        mean = jnp.broadcast_to(mm[0, pl.ds(r, 1), :], (8, 128))
        for j in (0, 8):
            a = jnp.where(narrow, la[r, j:j + 8, :], mean)
            packed_out[r, j:j + 8, :] = a
            dd[r + 2, j:j + 8, :] = a - pp[r, j:j + 8, :]
        prev = jnp.broadcast_to(mm[1, pl.ds(r, 1), :], (8, 128))
        follow = jnp.broadcast_to(mm[2, pl.ds(r, 1), :], (8, 128))
        dd[r + 2, 16:24, :] = jnp.where(sub < 4, follow, prev)
        return carry

    lax.fori_loop(0, ROWS, differ, 0, unroll=8)

    for side, wait, which in ((has_prev, la_up, (0, 1)), (has_next, la_down, (2, 3))):
        @pl.when(side)
        def _():
            wait.wait_recv()
            for i in which:
                mean = jnp.broadcast_to(mm[0, ROWS + i:ROWS + i + 1, :], (8, 128))
                for j in (0, 8):
                    a = jnp.where(narrow, la_in[i, j:j + 8, :], mean)
                    dd[i if i < 2 else ROWS + i, j:j + 8, :] = a

        @pl.when(jnp.logical_not(side))
        def _():
            for i in which:
                dd[i if i < 2 else ROWS + i, 0:16, :] = jnp.zeros((16, 128), F32)

    def correct(r, carry):
        t = [dd[r + 2, 8 * j:8 * j + 8, :] for j in range(3)]
        n1, n2 = around(*t, 1, sub), around(*t, 2, sub)
        p1, p2 = around(*t, -1, sub), around(*t, -2, sub)
        for j in range(2):
            at = slice(8 * j, 8 * j + 8)
            d = t[j]
            below = dd[r + 3, at, :]
            near = (n1[j] + p1[j]) + (dd[r + 1, at, :] + below)
            far = (n2[j] + p2[j]) + (dd[r, at, :] + dd[r + 4, at, :])
            lp1, lp2 = pltpu.roll(d, 1, 1), pltpu.roll(d, 2, 1)
            ln1, ln2 = pltpu.roll(d, 127, 1), pltpu.roll(d, 126, 1)
            base = (c0 * d + c1 * near) + (c2 * far + c_row * below)
            base = base + (c_cell * n1[j] + k1p * lp1) + (k1n * ln1 + k2p * lp2) + k2n * ln2
            side = (s1p * lp1 + s2p * lp2) + (s1n * ln1 + s2n * ln2)
            even[r, at, :] = jnp.where(is_even, base, side)
            odd[r, at, :] = jnp.where(is_even, side, base)
        return carry

    lax.fori_loop(0, ROWS, correct, 0, unroll=4)

    for d in FAR_FIRST:
        q_copy(d).wait_send()
        g_copy(d).wait_send()
    for copy in bulk + [edge_up, edge_down, edge_first, edge_last]:
        copy.wait_send()

    @pl.when(has_prev)
    def _():
        la_down.wait_send()
        for copy in down:
            copy.wait_send()
        for d in range(NZ):
            q_down(d).wait_send()

    @pl.when(has_next)
    def _():
        la_up.wait_send()
        for copy in up:
            copy.wait_send()
        for d in range(NZ):
            q_up(d).wait_send()


def run_exchange(widths, hydro, face, diffusion):
    dma = pltpu.SemaphoreType.DMA
    packed = jax.ShapeDtypeStruct((ROWS, CELLS, 128), F32)
    return pl.pallas_call(
        exchange,
        out_shape=(jax.ShapeDtypeStruct((FIELDS, ROWS, CELLS, THETA), F32), packed, packed, packed),
        in_specs=[pl.BlockSpec(memory_space=pltpu.HBM)] * 4,
        out_specs=(pl.BlockSpec(memory_space=pltpu.VMEM),) * 4,
        scratch_shapes=[
            pltpu.VMEM((NV, ROWS + 4, CELLS, THETA), F32),
            pltpu.VMEM((NF, ROWS, CELLS, THETA), F32),
            pltpu.VMEM((NV + 1, ROWS, 8, THETA), F32),
            pltpu.VMEM((NV + 1, 4, CELLS, THETA), F32),
            pltpu.VMEM((ROWS, CELLS, 128), F32),
            pltpu.VMEM((ROWS, CELLS, 128), F32),
            pltpu.VMEM((NZ, ROWS + 8, 128), F32),
            pltpu.VMEM((NG, ROWS + 8, 128), F32),
            pltpu.VMEM((4, ROWS, 128), F32),
            pltpu.VMEM((ROWS, 128), F32),
            pltpu.VMEM((ROWS, 128), F32),
            pltpu.VMEM((ROWS, 128), F32),
            pltpu.VMEM((ROWS, 128), F32),
            pltpu.VMEM((4, CELLS, 128), F32),
            pltpu.VMEM((ROWS + 4, CELLS + 8, 128), F32),
            pltpu.VMEM((3, ROWS + 8, 128), F32),
            pltpu.SMEM((16,), jnp.int32),
            pltpu.VMEM((NV, THETA), F32),
            dma((2,)),
            dma((8,)),
            dma((NZ,)), dma((NZ,)), dma((NZ,)), dma((NZ,)), dma((NZ,)), dma((NZ,)),
            dma((4,)), dma((4,)), dma((2,)), dma((2,)), dma((NG,)), dma((NG,)),
            dma((2 * NV + 1,)), dma((2 * NV + 1,)), dma((3,)), dma((3,)),
        ],
        compiler_params=pltpu.CompilerParams(
            collective_id=0, has_side_effects=True, vmem_limit_bytes=20 << 20
        ),
        name="exchange",
    )(*(pltpu.with_memory_space_constraint(x, pltpu.HBM) for x in (widths, hydro, face, diffusion)))


def update(pre, even, odd, packed, face, conserved, faces_out, co, fo, store_sem):
    lane = lanes((8, 128))

    def copy(f):
        return pltpu.make_async_copy(co.at[f], conserved.at[f], store_sem.at[f])

    def face_copy(k):
        return pltpu.make_async_copy(fo.at[k], faces_out.at[k], store_sem.at[FIELDS + k])

    for f in range(FIELDS):
        shift = (120 - 16 * f) % 128
        delta = even if f % 2 == 0 else odd

        def step(r, carry):
            for j in (0, 8):
                at = slice(j, j + 8)
                p = pltpu.roll(delta[r, at, :], shift, 1)
                co[f, r, at, 0:128] = pre[f, r, at, 0:128] + jnp.where(lane < 10, p, 0.0)
                co[f, r, at, 128:256] = pre[f, r, at, 128:256] + jnp.where(lane >= 118, p, 0.0)
                if f >= NV:
                    p = pltpu.roll(packed[r, at, :], shift, 1)
                    fo[f - NV, r, at, 0:128] = jnp.where(lane < 8, p, face[f - NV, r, at, 0:128])
                    fo[f - NV, r, at, 128:256] = jnp.where(lane >= 120, p, face[f - NV, r, at, 128:256])
            return carry

        lax.fori_loop(0, ROWS, step, 0, unroll=8)
        copy(f).start()
        if f >= NV:
            face_copy(f - NV).start()

    for f in range(FIELDS):
        copy(f).wait()
    for k in range(NF):
        face_copy(k).wait()


def run_update(pre, even, odd, packed, face):
    return pl.pallas_call(
        update,
        out_shape=(
            jax.ShapeDtypeStruct((FIELDS, ROWS, CELLS, THETA), F32),
            jax.ShapeDtypeStruct((NF, ROWS, CELLS, THETA), F32),
        ),
        in_specs=[pl.BlockSpec(memory_space=pltpu.VMEM)] * 5,
        out_specs=(pl.BlockSpec(memory_space=pltpu.HBM), pl.BlockSpec(memory_space=pltpu.HBM)),
        scratch_shapes=[
            pltpu.VMEM((FIELDS, ROWS, CELLS, THETA), F32),
            pltpu.VMEM((NF, ROWS, CELLS, THETA), F32),
            pltpu.SemaphoreType.DMA((FIELDS + NF,)),
        ],
        compiler_params=pltpu.CompilerParams(vmem_limit_bytes=16 << 20),
        name="update",
    )(pre, even, odd, packed, face)


def body(hydro, face, widths, diffusion):
    return run_update(*run_exchange(widths, hydro, face, diffusion), face)


def solution(mesh):
    spec = P(None, "row", "phi", None)
    return jax.shard_map(
        body, mesh=mesh, in_specs=(spec, spec, P(), P()), out_specs=(spec, spec), check_vma=False
    )
```

```python
import jax
import jax.numpy as jnp
from jax import lax
from jax.experimental import pallas as pl
from jax.experimental.pallas import tpu as pltpu
from jax.sharding import PartitionSpec as P

F32 = jnp.float32
MESH = pl.DeviceIdType.MESH
NV, NF, FIELDS = 5, 3, 8
ROWS, CELLS, THETA = 32, 16, 256
NZ, NG, NROW = 8, 8, 4
EARLY = 5
BATCH = 8
PART = 8
FAR_FIRST = (4, 3, 5, 2, 6, 1, 7)


def lanes(shape):
    return lax.broadcasted_iota(jnp.int32, shape, len(shape) - 1)


def sublanes(shape):
    return lax.broadcasted_iota(jnp.int32, shape, len(shape) - 2)


def around(t0, t1, h, k, sub):
    if k > 0:
        edge = sub >= 8 - k
        a, b, c = (None if t is None else pltpu.roll(t, 8 - k, 0) for t in (t0, t1, h))
        return jnp.where(edge, b, a), jnp.where(edge, 0.0 if c is None else c, b)
    edge = sub < -k
    a, b, c = (None if t is None else pltpu.roll(t, -k, 0) for t in (t0, t1, h))
    return jnp.where(edge, 0.0 if c is None else c, a), jnp.where(edge, a, b)


def exchange(
    widths_hbm, hydro, face, diffusion_hbm, pre, even, odd, packed_out,
    hv, fv, halo, radial, la, pp, zsum, gsum, edge, first, last, first_in, last_in, la_in,
    dd, mm, widths, diffusion, small_sem,
    load_sem, q_send, q_recv, qn_send, qn_recv, qp_send, qp_recv,
    la_send, la_recv, e_send, e_recv, g_send, g_recv,
    p_send, p_recv, r_send, r_recv,
):
    row, phi = lax.axis_index("row"), lax.axis_index("phi")
    z, g = phi % NZ, phi // NZ
    nphi = NZ * NG
    after, before = (phi + 1) % nphi, (phi + nphi - 1) % nphi
    has_prev, has_next = row > 0, row < NROW - 1

    def peer(d):
        return g * NZ + (z + d) % NZ

    def group(d):
        return ((g + d) % NG) * NZ + z

    get_widths = pltpu.make_async_copy(widths_hbm, widths, small_sem.at[0])
    get_diffusion = pltpu.make_async_copy(diffusion_hbm, diffusion, small_sem.at[1])
    get_widths.start()
    loads = []
    for i in range(4):
        loads.append((
            pltpu.make_async_copy(hydro.at[:, 8 * i:8 * i + 8], hv.at[:, 8 * i + 2:8 * i + 10], load_sem.at[2 * i]),
            pltpu.make_async_copy(face.at[:, 8 * i:8 * i + 8], fv.at[:, 8 * i:8 * i + 8], load_sem.at[2 * i + 1]),
        ))
        for copy in loads[i]:
            copy.start()
    get_diffusion.start()

    zsum[:, ROWS:, :] = jnp.zeros((NZ, 8, 128), F32)
    barrier = pltpu.get_barrier_semaphore()

    def hello(r, p):
        pl.semaphore_signal(barrier, inc=1, device_id=(r, p), device_id_type=MESH)

    for d in range(1, NZ):
        hello(row, peer(d))
        hello(row, group(d))

    @pl.when(has_prev)
    def _():
        for d in range(NZ):
            hello(row - 1, peer(d))

    @pl.when(has_next)
    def _():
        for d in range(NZ):
            hello(row + 1, peer(d))

    @pl.when(z == 0)
    def _():
        hello(row, before)

    @pl.when(z == NZ - 1)
    def _():
        hello(row, after)

    for i in range(NV):
        for r in (0, 1, ROWS + 2, ROWS + 3):
            hv[i, r] = jnp.zeros((CELLS, THETA), F32)

    lane = lanes((8, 128))
    sub = sublanes((8, 128))
    low = lane < 64
    get_widths.wait()
    width = jnp.zeros((8, 128), jnp.int32)
    for c in range(16):
        width = jnp.where(lane % 16 == c, widths[(c + 8) % 16], width)

    def pack(block, base):
        q8 = jnp.zeros((8, 128), F32)
        f8 = jnp.zeros((8, 128), F32)
        l8 = jnp.zeros((8, 128), F32)
        for i in range(8):
            r = block * 8 + i
            sums, local = [], []
            for j in range(2):
                p = None
                for f in range(FIELDS):
                    ref, k, at = (hv, f, r + 2) if f < NV else (fv, f - NV, r)
                    t0 = ref[k, at, 8 * j:8 * j + 8, 0:128]
                    t1 = ref[k, at, 8 * j:8 * j + 8, 128:256]
                    t = jnp.where(low, t0, t1)
                    shift = (8 + 16 * f) % 128
                    t = pltpu.roll(t, shift, 1)
                    p = t if p is None else jnp.where(lane // 16 == f, t, p)
                pp[r, 8 * j:8 * j + 8, :] = p
                s2 = p + jnp.where(sub % 2 == 0, pltpu.roll(p, 7, 0), pltpu.roll(p, 1, 0))
                s4 = s2 + jnp.where(sub % 4 < 2, pltpu.roll(s2, 6, 0), pltpu.roll(s2, 2, 0))
                s8 = s4 + pltpu.roll(s4, 4, 0)
                sums.append(s8)
                local.append((s2, s4, s8))
            s16 = sums[0] + sums[1]
            for j, (s2, s4, s8) in enumerate(local):
                mean = jnp.where(width == 2, s2 * 0.5, s16 * 0.0625)
                mean = jnp.where(width == 4, s4 * 0.25, mean)
                mean = jnp.where(width == 8, s8 * 0.125, mean)
                la[r, 8 * j:8 * j + 8, :] = mean
                local[j] = mean
            q8 = jnp.where(sub == i, s16, q8)
            f8 = jnp.where(sub == i, pltpu.roll(local[0], i, 0) if i else local[0], f8)
            l8 = jnp.where(sub == i, pltpu.roll(local[1], (i + 1) % 8, 0) if i < 7 else local[1], l8)
        at = pl.ds(pl.multiple_of(block * 8, 8), 8)
        zsum[z, at, :] = q8
        first[at, :] = f8
        last[at, :] = l8
        return base

    for i in range(4):
        for copy in loads[i]:
            copy.wait()
        pack(i, 0)

    hellos = 2 * (NZ - 1) + NZ * (has_prev.astype(jnp.int32) + has_next.astype(jnp.int32))
    hellos += (z == 0).astype(jnp.int32) + (z == NZ - 1).astype(jnp.int32)
    pl.semaphore_wait(barrier, hellos)

    def remote(src, dst, ssem, rsem, r, p):
        return pltpu.make_async_remote_copy(
            src_ref=src, dst_ref=dst, send_sem=ssem, recv_sem=rsem,
            device_id=(r, p), device_id_type=MESH,
        )

    def q_copy(d):
        ref = zsum.at[z, 0:ROWS, :]
        return remote(ref, ref, q_send.at[d], q_recv.at[d], row, peer(d))

    def q_down(d):
        return remote(
            zsum.at[z, 0:2, :], zsum.at[z, ROWS + 2:ROWS + 4, :],
            qn_send.at[d], qn_recv.at[d], row - 1, peer(d),
        )

    def q_up(d):
        return remote(
            zsum.at[z, ROWS - 2:ROWS, :], zsum.at[z, ROWS:ROWS + 2, :],
            qp_send.at[d], qp_recv.at[d], row + 1, peer(d),
        )

    for d in FAR_FIRST:
        q_copy(d).start()

    @pl.when(has_prev)
    def _():
        for d in FAR_FIRST + (0,):
            q_down(d).start()

    @pl.when(has_next)
    def _():
        for d in FAR_FIRST + (0,):
            q_up(d).start()

    edge_first = remote(first, first_in, la_send.at[0], la_recv.at[0], row, before)
    edge_last = remote(last, last_in, la_send.at[1], la_recv.at[1], row, after)
    edge_first.start()
    edge_last.start()
    la_down = remote(la.at[0:2], la_in.at[2:4], la_send.at[2], la_recv.at[2], row - 1, phi)
    la_up = remote(la.at[ROWS - 2:ROWS], la_in.at[0:2], la_send.at[3], la_recv.at[3], row + 1, phi)

    down = [remote(hv.at[:, 2:4], radial.at[0:NV, 2:4], r_send.at[0], r_recv.at[0], row - 1, phi)]
    down += [remote(fv.at[0, 0:1], radial.at[NV, 2:3], r_send.at[1], r_recv.at[1], row - 1, phi)]
    up = [remote(hv.at[:, ROWS:ROWS + 2], radial.at[0:NV, 0:2], r_send.at[2], r_recv.at[2], row + 1, phi)]

    @pl.when(has_prev)
    def _():
        la_down.start()
        for copy in down:
            copy.start()

    @pl.when(has_next)
    def _():
        la_up.start()
        for copy in up:
            copy.start()

    bulk = []
    for i in range(NV):
        bulk.append(remote(
            hv.at[i, 2:ROWS + 2, CELLS - 2:CELLS, :], halo.at[i, :, 6:8, :],
            p_send.at[2 * i], p_recv.at[2 * i], row, after,
        ))
        bulk.append(remote(
            hv.at[i, 2:ROWS + 2, 0:2, :], halo.at[i, :, 0:2, :],
            p_send.at[2 * i + 1], p_recv.at[2 * i + 1], row, before,
        ))
    bulk.append(remote(
        fv.at[2, :, 0:1, :], halo.at[NV, :, 0:1, :],
        p_send.at[2 * NV], p_recv.at[2 * NV], row, before,
    ))
    for copy in bulk[:2 * EARLY]:
        copy.start()

    get_diffusion.wait()
    i0 = lax.broadcasted_iota(jnp.int32, (THETA, THETA), 0)
    i1 = lax.broadcasted_iota(jnp.int32, (THETA, THETA), 1)
    apart = jnp.abs(i0 - i1)
    band = jnp.where(apart == 0, -90.0, jnp.where(apart == 1, 16.0, jnp.where(apart == 2, -1.0, 0.0)))
    band = band.astype(jnp.bfloat16)

    def raw_field(f):
        diff = diffusion[f:f + 1, :] * (1.0 / 12.0)

        def step(block, carry):
            r0 = block * BATCH
            centre = jnp.concatenate([hv[f, r0 + i + 2] for i in range(BATCH)], 0)
            high = centre.astype(jnp.bfloat16)
            rest = (centre - high.astype(F32)).astype(jnp.bfloat16)
            theta = jnp.dot(high, band, preferred_element_type=F32)
            theta = theta + jnp.dot(rest, band, preferred_element_type=F32)
            for i in range(BATCH):
                r = r0 + i + 2
                for half in range(2):
                    ln = slice(128 * half, 128 * half + 128)
                    t = [hv[f, r, 8 * j:8 * j + 8, ln] for j in range(2)] + [None]
                    n1, n2 = around(*t, 1, sub), around(*t, 2, sub)
                    p1, p2 = around(*t, -1, sub), around(*t, -2, sub)
                    for j in range(2):
                        at = slice(8 * j, 8 * j + 8)
                        near = (n1[j] + p1[j]) + (hv[f, r - 1, at, ln] + hv[f, r + 1, at, ln])
                        far = (n2[j] + p2[j]) + (hv[f, r - 2, at, ln] + hv[f, r + 2, at, ln])
                        change = 16.0 * near - far
                        change = change + theta[16 * i + 8 * j:16 * i + 8 * j + 8, ln]
                        pre[f, r0 + i, at, ln] = t[j] + diff[:, ln] * change
            return carry

        lax.fori_loop(0, ROWS // BATCH, step, 0)

    def raw_faces():
        def step(r, carry):
            for j in (0, 8):
                a, b = fv[1, r, j:j + 8, 0:128], fv[1, r, j:j + 8, 128:256]
                ra, rb = pltpu.roll(a, 127, 1), pltpu.roll(b, 127, 1)
                pre[NV + 1, r, j:j + 8, 0:128] = 0.5 * (a + jnp.where(lane == 127, rb, ra))
                pre[NV + 1, r, j:j + 8, 128:256] = 0.5 * (b + jnp.where(lane == 127, 0.0, rb))
            for half in range(2):
                ln = slice(128 * half, 128 * half + 128)
                t = [fv[2, r, 8 * j:8 * j + 8, ln] for j in range(2)]
                n1 = around(t[0], t[1], None, 1, sub)
                for j in range(2):
                    pre[NV + 2, r, 8 * j:8 * j + 8, ln] = 0.5 * (t[j] + n1[j])
            return carry
        lax.fori_loop(0, ROWS, step, 0, unroll=4)

        def mean_step(r, carry):
            pre[NV, r] = 0.5 * (fv[0, r] + fv[0, r + 1])
            return carry
        lax.fori_loop(0, ROWS - 1, mean_step, 0)
        pre[NV, ROWS - 1] = 0.5 * fv[0, ROWS - 1]

    for f in range(NV):
        raw_field(f)

    for d in FAR_FIRST:
        q_copy(d).wait_recv()

    @pl.when(has_prev)
    def _():
        for d in FAR_FIRST + (0,):
            q_up(d).wait_recv()

    @pl.when(has_next)
    def _():
        for d in FAR_FIRST + (0,):
            q_down(d).wait_recv()

    def z_sums(at):
        pair, quad = (at // 2) * 2, (at // 4) * 4
        s32 = zsum[pair] + zsum[pair + 1]
        s64 = (zsum[quad] + zsum[quad + 1]) + (zsum[quad + 2] + zsum[quad + 3])
        return s32, s64

    tall = (ROWS + 8, 128)
    wide = jnp.broadcast_to(width[0:1], tall)
    total = zsum[0]
    for i in range(1, NZ):
        total = total + zsum[i]
    gsum[g] = total

    def g_copy(d):
        return remote(gsum.at[g], gsum.at[g], g_send.at[d], g_recv.at[d], row, group(d))

    for d in (5, 3, 7, 1, 6, 2, 4):
        g_copy(d).start()

    s32p, s64p = z_sums((z + NZ - 1) % NZ)
    s32n, s64n = z_sums((z + 1) % NZ)
    edge[0] = jnp.where(wide == 32, s32p * (1 / 32), s64p * (1 / 64))[:ROWS]
    edge[1] = jnp.where(wide == 32, s32n * (1 / 32), s64n * (1 / 64))[:ROWS]
    edge_up = remote(edge.at[0], edge.at[2], e_send.at[0], e_recv.at[0], row, group(1))
    edge_down = remote(edge.at[1], edge.at[3], e_send.at[1], e_recv.at[1], row, group(NG - 1))

    @pl.when(z == 0)
    def _():
        edge_up.start()

    @pl.when(z == NZ - 1)
    def _():
        edge_down.start()

    for copy in bulk[2 * EARLY:]:
        copy.start()

    raw_faces()

    seg, m = lane // 16, lane % 16
    is_even = seg % 2 == 0
    diff_even = jnp.zeros((8, 128), F32)
    diff_odd = jnp.zeros((8, 128), F32)
    for f in range(NV):
        t = jnp.where(low, diffusion[f:f + 1, 0:128], diffusion[f:f + 1, 128:256])
        t = pltpu.roll(jnp.broadcast_to(t, (8, 128)), (8 + 16 * f) % 128, 1) * (1.0 / 12.0)
        near_f = (lane - 16 * f + 2 + 128) % 128 < 20
        if f % 2 == 0:
            diff_even = jnp.where(near_f, t, diff_even)
        else:
            diff_odd = jnp.where(near_f, t, diff_odd)
    own = jnp.where(is_even, diff_even, diff_odd)
    out = jnp.where(is_even, diff_odd, diff_even)
    fluid = seg < NV
    zero = jnp.zeros((8, 128), F32)
    c0 = jnp.where(fluid, 1.0 - 90.0 * own, 0.5)
    c1 = jnp.where(fluid, 16.0 * own, zero)
    c2 = jnp.where(fluid, -own, zero)
    c_row = jnp.where(seg == NV, 0.5, zero)
    c_cell = jnp.where(seg == NV + 2, 0.5, zero)
    k1p = jnp.where(m % 8 == 0, zero, c1)
    k1n = jnp.where(m % 8 == 7, zero, c1 + jnp.where(seg == NV + 1, 0.5, zero))
    k2p = jnp.where(m % 8 < 2, zero, c2)
    k2n = jnp.where(m % 8 > 5, zero, c2)
    from_left = (seg + 7) % 8
    from_right = (seg + 1) % 8
    left_fluid, right_fluid = from_left < NV, from_right < NV
    s1p = jnp.where(jnp.logical_and(m == 0, left_fluid), 16.0 * out, zero)
    s2p = jnp.where(jnp.logical_and(m < 2, left_fluid), -out, zero)
    s1n = jnp.where(jnp.logical_and(m == 15, right_fluid), 16.0 * out, zero)
    s1n = jnp.where(jnp.logical_and(m == 15, from_right == NV + 1), 0.5, s1n)
    s2n = jnp.where(jnp.logical_and(m > 13, right_fluid), -out, zero)

    inner = (lane >= 8, lane < 120)

    @pl.when(has_prev)
    def _():
        for copy in up:
            copy.wait_recv()
        for f in range(NV):
            for half in range(2):
                ln = slice(128 * half, 128 * half + 128)
                diff = diffusion[f:f + 1, ln] * (1.0 / 12.0)
                for at in (slice(0, 8), slice(8, 16)):
                    b2, b1 = (jnp.where(inner[half], radial[f, i, at, ln], 0.0) for i in (0, 1))
                    pre[f, 0, at, ln] = pre[f, 0, at, ln] + diff * (16.0 * b1 - b2)
                    pre[f, 1, at, ln] = pre[f, 1, at, ln] - diff * b1

    @pl.when(has_next)
    def _():
        for copy in down:
            copy.wait_recv()
        for half in range(2):
            ln = slice(128 * half, 128 * half + 128)
            for at in (slice(0, 8), slice(8, 16)):
                for f in range(NV):
                    diff = diffusion[f:f + 1, ln] * (1.0 / 12.0)
                    b1, b2 = (jnp.where(inner[half], radial[f, i, at, ln], 0.0) for i in (2, 3))
                    e, e1 = ROWS - 1, ROWS - 2
                    pre[f, e, at, ln] = pre[f, e, at, ln] + diff * (16.0 * b1 - b2)
                    pre[f, e1, at, ln] = pre[f, e1, at, ln] - diff * b1
                b = jnp.where(inner[half], radial[NV, 2, at, ln], 0.0)
                pre[NV, ROWS - 1, at, ln] = pre[NV, ROWS - 1, at, ln] + 0.5 * b

    a1 = jnp.where(sub == 0, 16.0, zero)
    a2 = jnp.where(sub < 2, -1.0, zero)
    b1 = jnp.where(sub == 7, 16.0, zero)
    b2 = jnp.where(sub > 5, -1.0, zero)
    for f in range(NV):
        bulk[2 * f].wait_recv()
        bulk[2 * f + 1].wait_recv()
        diffs = [diffusion[f:f + 1, 128 * half:128 * half + 128] * (1.0 / 12.0) for half in range(2)]

        def step(r, carry):
            for half in range(2):
                ln = slice(128 * half, 128 * half + 128)
                h = jnp.where(inner[half], halo[f, r, :, ln], 0.0) * diffs[half]
                head = a1 * pltpu.roll(h, 1, 0) + a2 * pltpu.roll(h, 2, 0)
                tail = b1 * pltpu.roll(h, 7, 0) + b2 * pltpu.roll(h, 6, 0)
                pre[f, r, 0:8, ln] = pre[f, r, 0:8, ln] + head
                pre[f, r, 8:16, ln] = pre[f, r, 8:16, ln] + tail
            return carry
        lax.fori_loop(0, ROWS, step, 0, unroll=8)
    bulk[2 * NV].wait_recv()

    def face_step(r, carry):
        for half in range(2):
            ln = slice(128 * half, 128 * half + 128)
            h = pltpu.roll(halo[NV, r, :, ln], 7, 0)
            h = jnp.where(jnp.logical_and(inner[half], sub == 7), 0.5 * h, 0.0)
            pre[NV + 2, r, 8:16, ln] = pre[NV + 2, r, 8:16, ln] + h
        return carry
    lax.fori_loop(0, ROWS, face_step, 0, unroll=8)

    for d in (5, 3, 7, 1, 6, 2, 4):
        g_copy(d).wait_recv()

    @pl.when(z == 0)
    def _():
        edge_up.wait_recv()
        edge_up.wait_send()

    @pl.when(z == NZ - 1)
    def _():
        edge_down.wait_recv()
        edge_down.wait_send()

    edge_first.wait_recv()
    edge_last.wait_recv()

    whole = gsum[0]
    for i in range(1, NG):
        whole = whole + gsum[i]
    whole = whole * (1 / 1024)

    def g_means(at, small):
        pair, quad = (at // 2) * 2, (at // 4) * 4
        mean = jnp.where(wide == 128, gsum[at] * (1 / 128), small)
        mean = jnp.where(wide == 256, (gsum[pair] + gsum[pair + 1]) * (1 / 256), mean)
        four = (gsum[quad] + gsum[quad + 1]) + (gsum[quad + 2] + gsum[quad + 3])
        mean = jnp.where(wide == 512, four * (1 / 512), mean)
        return jnp.where(wide == 1024, whole, mean)

    s32, s64 = z_sums(z)
    mm[0] = g_means(g, jnp.where(wide == 32, s32 * (1 / 32), s64 * (1 / 64)))
    gp = jnp.where(z == 0, (g + NG - 1) % NG, g)
    gn = jnp.where(z == NZ - 1, (g + 1) % NG, g)
    pad = jnp.zeros((8, 128), F32)
    ep = jnp.concatenate([jnp.where(z == 0, edge[2], edge[0]), pad])
    en = jnp.concatenate([jnp.where(z == NZ - 1, edge[3], edge[1]), pad])
    mm[1] = jnp.where(wide <= 16, jnp.concatenate([last_in[...], pad]), g_means(gp, ep))
    mm[2] = jnp.where(wide <= 16, jnp.concatenate([first_in[...], pad]), g_means(gn, en))
    narrow = width <= 16

    def differ(r, carry):
        mean = jnp.broadcast_to(mm[0, pl.ds(r, 1), :], (8, 128))
        for j in (0, 8):
            a = jnp.where(narrow, la[r, j:j + 8, :], mean)
            packed_out[r, j:j + 8, :] = a
            dd[r + 2, j:j + 8, :] = a - pp[r, j:j + 8, :]
        prev = jnp.broadcast_to(mm[1, pl.ds(r, 1), :], (8, 128))
        follow = jnp.broadcast_to(mm[2, pl.ds(r, 1), :], (8, 128))
        dd[r + 2, 16:24, :] = jnp.where(sub < 4, follow, prev)
        return carry

    lax.fori_loop(0, ROWS, differ, 0, unroll=8)

    for side, wait, which in ((has_prev, la_up, (0, 1)), (has_next, la_down, (2, 3))):
        @pl.when(side)
        def _():
            wait.wait_recv()
            for i in which:
                mean = jnp.broadcast_to(mm[0, ROWS + i:ROWS + i + 1, :], (8, 128))
                for j in (0, 8):
                    a = jnp.where(narrow, la_in[i, j:j + 8, :], mean)
                    dd[i if i < 2 else ROWS + i, j:j + 8, :] = a

        @pl.when(jnp.logical_not(side))
        def _():
            for i in which:
                dd[i if i < 2 else ROWS + i, 0:16, :] = jnp.zeros((16, 128), F32)

    def correct(r, carry):
        t = [dd[r + 2, 8 * j:8 * j + 8, :] for j in range(3)]
        n1, n2 = around(*t, 1, sub), around(*t, 2, sub)
        p1, p2 = around(*t, -1, sub), around(*t, -2, sub)
        for j in range(2):
            at = slice(8 * j, 8 * j + 8)
            d = t[j]
            below = dd[r + 3, at, :]
            near = (n1[j] + p1[j]) + (dd[r + 1, at, :] + below)
            far = (n2[j] + p2[j]) + (dd[r, at, :] + dd[r + 4, at, :])
            lp1, lp2 = pltpu.roll(d, 1, 1), pltpu.roll(d, 2, 1)
            ln1, ln2 = pltpu.roll(d, 127, 1), pltpu.roll(d, 126, 1)
            base = (c0 * d + c1 * near) + (c2 * far + c_row * below)
            base = base + (c_cell * n1[j] + k1p * lp1) + (k1n * ln1 + k2p * lp2) + k2n * ln2
            side = (s1p * lp1 + s2p * lp2) + (s1n * ln1 + s2n * ln2)
            even[r, at, :] = jnp.where(is_even, base, side)
            odd[r, at, :] = jnp.where(is_even, side, base)
        return carry

    lax.fori_loop(0, ROWS, correct, 0, unroll=4)

    for d in FAR_FIRST:
        q_copy(d).wait_send()
        g_copy(d).wait_send()
    for copy in bulk + [edge_first, edge_last]:
        copy.wait_send()

    @pl.when(has_prev)
    def _():
        la_down.wait_send()
        for copy in down:
            copy.wait_send()
        for d in range(NZ):
            q_down(d).wait_send()

    @pl.when(has_next)
    def _():
        la_up.wait_send()
        for copy in up:
            copy.wait_send()
        for d in range(NZ):
            q_up(d).wait_send()


def run_exchange(widths, hydro, face, diffusion):
    dma = pltpu.SemaphoreType.DMA
    packed = jax.ShapeDtypeStruct((ROWS, CELLS, 128), F32)
    return pl.pallas_call(
        exchange,
        out_shape=(jax.ShapeDtypeStruct((FIELDS, ROWS, CELLS, THETA), F32), packed, packed, packed),
        in_specs=[pl.BlockSpec(memory_space=pltpu.HBM)] * 4,
        out_specs=(pl.BlockSpec(memory_space=pltpu.VMEM),) * 4,
        scratch_shapes=[
            pltpu.VMEM((NV, ROWS + 4, CELLS, THETA), F32),
            pltpu.VMEM((NF, ROWS, CELLS, THETA), F32),
            pltpu.VMEM((NV + 1, ROWS, 8, THETA), F32),
            pltpu.VMEM((NV + 1, 4, CELLS, THETA), F32),
            pltpu.VMEM((ROWS, CELLS, 128), F32),
            pltpu.VMEM((ROWS, CELLS, 128), F32),
            pltpu.VMEM((NZ, ROWS + 8, 128), F32),
            pltpu.VMEM((NG, ROWS + 8, 128), F32),
            pltpu.VMEM((4, ROWS, 128), F32),
            pltpu.VMEM((ROWS, 128), F32),
            pltpu.VMEM((ROWS, 128), F32),
            pltpu.VMEM((ROWS, 128), F32),
            pltpu.VMEM((ROWS, 128), F32),
            pltpu.VMEM((4, CELLS, 128), F32),
            pltpu.VMEM((ROWS + 4, CELLS + 8, 128), F32),
            pltpu.VMEM((3, ROWS + 8, 128), F32),
            pltpu.SMEM((16,), jnp.int32),
            pltpu.VMEM((NV, THETA), F32),
            dma((2,)),
            dma((8,)),
            dma((NZ,)), dma((NZ,)), dma((NZ,)), dma((NZ,)), dma((NZ,)), dma((NZ,)),
            dma((4,)), dma((4,)), dma((2,)), dma((2,)), dma((NG,)), dma((NG,)),
            dma((2 * NV + 1,)), dma((2 * NV + 1,)), dma((3,)), dma((3,)),
        ],
        compiler_params=pltpu.CompilerParams(
            collective_id=0, has_side_effects=True, vmem_limit_bytes=20 << 20
        ),
        name="exchange",
    )(*(pltpu.with_memory_space_constraint(x, pltpu.HBM) for x in (widths, hydro, face, diffusion)))


def update(pre, even, odd, packed, face, conserved, faces_out, co, fo, store_sem):
    lane = lanes((8, 128))

    def stores(f, part):
        at = pl.ds(PART * part, PART)
        out = [pltpu.make_async_copy(co.at[f, at], conserved.at[f, at], store_sem.at[f, part])]
        if f >= NV:
            k = f - NV
            out.append(pltpu.make_async_copy(fo.at[k, at], faces_out.at[k, at], store_sem.at[FIELDS + k, part]))
        return out

    order = (5, 6, 7, 0, 1, 2, 3, 4)
    for f in order:
        shift = (120 - 16 * f) % 128
        delta = even if f % 2 == 0 else odd

        def step(r, carry):
            for j in (0, 8):
                at = slice(j, j + 8)
                p = pltpu.roll(delta[r, at, :], shift, 1)
                co[f, r, at, 0:128] = pre[f, r, at, 0:128] + jnp.where(lane < 10, p, 0.0)
                co[f, r, at, 128:256] = pre[f, r, at, 128:256] + jnp.where(lane >= 118, p, 0.0)
                if f >= NV:
                    p = pltpu.roll(packed[r, at, :], shift, 1)
                    fo[f - NV, r, at, 0:128] = jnp.where(lane < 8, p, face[f - NV, r, at, 0:128])
                    fo[f - NV, r, at, 128:256] = jnp.where(lane >= 120, p, face[f - NV, r, at, 128:256])
            return carry

        for part in range(ROWS // PART):
            lax.fori_loop(PART * part, PART * part + PART, step, 0, unroll=8)
            for store in stores(f, part):
                store.start()

    for f in order:
        for part in range(ROWS // PART):
            for store in stores(f, part):
                store.wait()


def run_update(pre, even, odd, packed, face):
    return pl.pallas_call(
        update,
        out_shape=(
            jax.ShapeDtypeStruct((FIELDS, ROWS, CELLS, THETA), F32),
            jax.ShapeDtypeStruct((NF, ROWS, CELLS, THETA), F32),
        ),
        in_specs=[pl.BlockSpec(memory_space=pltpu.VMEM)] * 5,
        out_specs=(pl.BlockSpec(memory_space=pltpu.HBM), pl.BlockSpec(memory_space=pltpu.HBM)),
        scratch_shapes=[
            pltpu.VMEM((FIELDS, ROWS, CELLS, THETA), F32),
            pltpu.VMEM((NF, ROWS, CELLS, THETA), F32),
            pltpu.SemaphoreType.DMA((FIELDS + NF, ROWS // PART)),
        ],
        compiler_params=pltpu.CompilerParams(vmem_limit_bytes=16 << 20),
        name="update",
    )(pre, even, odd, packed, face)


def body(hydro, face, widths, diffusion):
    return run_update(*run_exchange(widths, hydro, face, diffusion), face)


def solution(mesh):
    spec = P(None, "row", "phi", None)
    return jax.shard_map(
        body, mesh=mesh, in_specs=(spec, spec, P(), P()), out_specs=(spec, spec), check_vma=False
    )
```

```python
import jax
import jax.numpy as jnp
from jax import lax
from jax.experimental import pallas as pl
from jax.experimental.pallas import tpu as pltpu
from jax.sharding import PartitionSpec as P

F32 = jnp.float32
MESH = pl.DeviceIdType.MESH
NV, NF, FIELDS = 5, 3, 8
ROWS, CELLS, THETA = 32, 16, 256
NZ, NG, NROW = 8, 8, 4
EARLY = 5
BATCH = 8
PART = 8
G_ORDER = (5, 3, 7, 1, 6, 2, 4)
FAR_FIRST = (4, 3, 5, 2, 6, 1, 7)


def lanes(shape):
    return lax.broadcasted_iota(jnp.int32, shape, len(shape) - 1)


def sublanes(shape):
    return lax.broadcasted_iota(jnp.int32, shape, len(shape) - 2)


def around(t0, t1, h, k, sub):
    if k > 0:
        edge = sub >= 8 - k
        a, b, c = (None if t is None else pltpu.roll(t, 8 - k, 0) for t in (t0, t1, h))
        return jnp.where(edge, b, a), jnp.where(edge, 0.0 if c is None else c, b)
    edge = sub < -k
    a, b, c = (None if t is None else pltpu.roll(t, -k, 0) for t in (t0, t1, h))
    return jnp.where(edge, 0.0 if c is None else c, a), jnp.where(edge, a, b)


def exchange(
    widths_hbm, hydro, face, diffusion_hbm, pre, even, odd, packed_out,
    hv, fv, halo, radial, la, pp, zsum, gsum, edge, first, last, first_in, last_in, la_in,
    dd, mm, widths, diffusion, small_sem,
    load_sem, q_send, q_recv, qn_send, qn_recv, qp_send, qp_recv,
    la_send, la_recv, e_send, e_recv, g_send, g_recv,
    p_send, p_recv, r_send, r_recv, fed, f_sem,
):
    row, phi = lax.axis_index("row"), lax.axis_index("phi")
    z, g = phi % NZ, phi // NZ
    nphi = NZ * NG
    after, before = (phi + 1) % nphi, (phi + nphi - 1) % nphi
    has_prev, has_next = row > 0, row < NROW - 1

    at_seam = jnp.logical_or(z == 0, z == NZ - 1)
    feeder = jnp.logical_or(z == 1, z == NZ - 2)
    beside = g * NZ + z + 1 - 2 * (z % 2)
    off_seam = jnp.logical_not(at_seam)

    def peer(d):
        return g * NZ + (z + d) % NZ

    def group(d):
        return ((g + d) % NG) * NZ + z

    get_widths = pltpu.make_async_copy(widths_hbm, widths, small_sem.at[0])
    get_diffusion = pltpu.make_async_copy(diffusion_hbm, diffusion, small_sem.at[1])
    get_widths.start()
    loads = []
    for i in range(4):
        loads.append((
            pltpu.make_async_copy(hydro.at[:, 8 * i:8 * i + 8], hv.at[:, 8 * i + 2:8 * i + 10], load_sem.at[2 * i]),
            pltpu.make_async_copy(face.at[:, 8 * i:8 * i + 8], fv.at[:, 8 * i:8 * i + 8], load_sem.at[2 * i + 1]),
        ))
        for copy in loads[i]:
            copy.start()
    get_diffusion.start()

    zsum[:, ROWS:, :] = jnp.zeros((NZ, 8, 128), F32)
    barrier = pltpu.get_barrier_semaphore()

    def hello(r, p):
        pl.semaphore_signal(barrier, inc=1, device_id=(r, p), device_id_type=MESH)

    for d in range(1, NZ):
        hello(row, peer(d))

    @pl.when(off_seam)
    def _():
        for d in range(1, NG):
            hello(row, group(d))

    @pl.when(has_prev)
    def _():
        for d in range(NZ):
            hello(row - 1, peer(d))

    @pl.when(has_next)
    def _():
        for d in range(NZ):
            hello(row + 1, peer(d))

    @pl.when(z == 0)
    def _():
        hello(row, before)

    @pl.when(z == NZ - 1)
    def _():
        hello(row, after)

    for i in range(NV):
        for r in (0, 1, ROWS + 2, ROWS + 3):
            hv[i, r] = jnp.zeros((CELLS, THETA), F32)

    lane = lanes((8, 128))
    sub = sublanes((8, 128))
    low = lane < 64
    get_widths.wait()
    width = jnp.zeros((8, 128), jnp.int32)
    for c in range(16):
        width = jnp.where(lane % 16 == c, widths[(c + 8) % 16], width)

    def pack(block, base):
        q8 = jnp.zeros((8, 128), F32)
        f8 = jnp.zeros((8, 128), F32)
        l8 = jnp.zeros((8, 128), F32)
        for i in range(8):
            r = block * 8 + i
            sums, local = [], []
            for j in range(2):
                p = None
                for f in range(FIELDS):
                    ref, k, at = (hv, f, r + 2) if f < NV else (fv, f - NV, r)
                    t0 = ref[k, at, 8 * j:8 * j + 8, 0:128]
                    t1 = ref[k, at, 8 * j:8 * j + 8, 128:256]
                    t = jnp.where(low, t0, t1)
                    shift = (8 + 16 * f) % 128
                    t = pltpu.roll(t, shift, 1)
                    p = t if p is None else jnp.where(lane // 16 == f, t, p)
                pp[r, 8 * j:8 * j + 8, :] = p
                s2 = p + jnp.where(sub % 2 == 0, pltpu.roll(p, 7, 0), pltpu.roll(p, 1, 0))
                s4 = s2 + jnp.where(sub % 4 < 2, pltpu.roll(s2, 6, 0), pltpu.roll(s2, 2, 0))
                s8 = s4 + pltpu.roll(s4, 4, 0)
                sums.append(s8)
                local.append((s2, s4, s8))
            s16 = sums[0] + sums[1]
            for j, (s2, s4, s8) in enumerate(local):
                mean = jnp.where(width == 2, s2 * 0.5, s16 * 0.0625)
                mean = jnp.where(width == 4, s4 * 0.25, mean)
                mean = jnp.where(width == 8, s8 * 0.125, mean)
                la[r, 8 * j:8 * j + 8, :] = mean
                local[j] = mean
            q8 = jnp.where(sub == i, s16, q8)
            f8 = jnp.where(sub == i, pltpu.roll(local[0], i, 0) if i else local[0], f8)
            l8 = jnp.where(sub == i, pltpu.roll(local[1], (i + 1) % 8, 0) if i < 7 else local[1], l8)
        at = pl.ds(pl.multiple_of(block * 8, 8), 8)
        zsum[z, at, :] = q8
        first[at, :] = f8
        last[at, :] = l8
        return base

    for i in range(4):
        for copy in loads[i]:
            copy.wait()
        pack(i, 0)

    hellos = (NZ - 1) + (NG - 1) * off_seam.astype(jnp.int32) + NZ * (has_prev.astype(jnp.int32) + has_next.astype(jnp.int32))
    hellos += (z == 0).astype(jnp.int32) + (z == NZ - 1).astype(jnp.int32)
    pl.semaphore_wait(barrier, hellos)

    def remote(src, dst, ssem, rsem, r, p):
        return pltpu.make_async_remote_copy(
            src_ref=src, dst_ref=dst, send_sem=ssem, recv_sem=rsem,
            device_id=(r, p), device_id_type=MESH,
        )

    def q_copy(d):
        ref = zsum.at[z, 0:ROWS, :]
        return remote(ref, ref, q_send.at[d], q_recv.at[d], row, peer(d))

    def q_down(d):
        return remote(
            zsum.at[z, 0:2, :], zsum.at[z, ROWS + 2:ROWS + 4, :],
            qn_send.at[d], qn_recv.at[d], row - 1, peer(d),
        )

    def q_up(d):
        return remote(
            zsum.at[z, ROWS - 2:ROWS, :], zsum.at[z, ROWS:ROWS + 2, :],
            qp_send.at[d], qp_recv.at[d], row + 1, peer(d),
        )

    for d in FAR_FIRST:
        q_copy(d).start()

    @pl.when(has_prev)
    def _():
        for d in FAR_FIRST + (0,):
            q_down(d).start()

    @pl.when(has_next)
    def _():
        for d in FAR_FIRST + (0,):
            q_up(d).start()

    edge_first = remote(first, first_in, la_send.at[0], la_recv.at[0], row, before)
    edge_last = remote(last, last_in, la_send.at[1], la_recv.at[1], row, after)
    edge_first.start()
    edge_last.start()
    la_down = remote(la.at[0:2], la_in.at[2:4], la_send.at[2], la_recv.at[2], row - 1, phi)
    la_up = remote(la.at[ROWS - 2:ROWS], la_in.at[0:2], la_send.at[3], la_recv.at[3], row + 1, phi)

    down = [remote(hv.at[:, 2:4], radial.at[0:NV, 2:4], r_send.at[0], r_recv.at[0], row - 1, phi)]
    down += [remote(fv.at[0, 0:1], radial.at[NV, 2:3], r_send.at[1], r_recv.at[1], row - 1, phi)]
    up = [remote(hv.at[:, ROWS:ROWS + 2], radial.at[0:NV, 0:2], r_send.at[2], r_recv.at[2], row + 1, phi)]

    @pl.when(has_prev)
    def _():
        la_down.start()
        for copy in down:
            copy.start()

    @pl.when(has_next)
    def _():
        la_up.start()
        for copy in up:
            copy.start()

    bulk = []
    for i in range(NV):
        bulk.append(remote(
            hv.at[i, 2:ROWS + 2, CELLS - 2:CELLS, :], halo.at[i, :, 6:8, :],
            p_send.at[2 * i], p_recv.at[2 * i], row, after,
        ))
        bulk.append(remote(
            hv.at[i, 2:ROWS + 2, 0:2, :], halo.at[i, :, 0:2, :],
            p_send.at[2 * i + 1], p_recv.at[2 * i + 1], row, before,
        ))
    bulk.append(remote(
        fv.at[2, :, 0:1, :], halo.at[NV, :, 0:1, :],
        p_send.at[2 * NV], p_recv.at[2 * NV], row, before,
    ))
    for copy in bulk[:2 * EARLY]:
        copy.start()

    get_diffusion.wait()
    i0 = lax.broadcasted_iota(jnp.int32, (THETA, THETA), 0)
    i1 = lax.broadcasted_iota(jnp.int32, (THETA, THETA), 1)
    apart = jnp.abs(i0 - i1)
    band = jnp.where(apart == 0, -90.0, jnp.where(apart == 1, 16.0, jnp.where(apart == 2, -1.0, 0.0)))
    band = band.astype(jnp.bfloat16)

    def raw_field(f):
        diff = diffusion[f:f + 1, :] * (1.0 / 12.0)

        def step(block, carry):
            r0 = block * BATCH
            centre = jnp.concatenate([hv[f, r0 + i + 2] for i in range(BATCH)], 0)
            high = centre.astype(jnp.bfloat16)
            rest = (centre - high.astype(F32)).astype(jnp.bfloat16)
            theta = jnp.dot(high, band, preferred_element_type=F32)
            theta = theta + jnp.dot(rest, band, preferred_element_type=F32)
            for i in range(BATCH):
                r = r0 + i + 2
                for half in range(2):
                    ln = slice(128 * half, 128 * half + 128)
                    t = [hv[f, r, 8 * j:8 * j + 8, ln] for j in range(2)] + [None]
                    n1, n2 = around(*t, 1, sub), around(*t, 2, sub)
                    p1, p2 = around(*t, -1, sub), around(*t, -2, sub)
                    for j in range(2):
                        at = slice(8 * j, 8 * j + 8)
                        near = (n1[j] + p1[j]) + (hv[f, r - 1, at, ln] + hv[f, r + 1, at, ln])
                        far = (n2[j] + p2[j]) + (hv[f, r - 2, at, ln] + hv[f, r + 2, at, ln])
                        change = 16.0 * near - far
                        change = change + theta[16 * i + 8 * j:16 * i + 8 * j + 8, ln]
                        pre[f, r0 + i, at, ln] = t[j] + diff[:, ln] * change
            return carry

        lax.fori_loop(0, ROWS // BATCH, step, 0)

    def raw_faces():
        def step(r, carry):
            for j in (0, 8):
                a, b = fv[1, r, j:j + 8, 0:128], fv[1, r, j:j + 8, 128:256]
                ra, rb = pltpu.roll(a, 127, 1), pltpu.roll(b, 127, 1)
                pre[NV + 1, r, j:j + 8, 0:128] = 0.5 * (a + jnp.where(lane == 127, rb, ra))
                pre[NV + 1, r, j:j + 8, 128:256] = 0.5 * (b + jnp.where(lane == 127, 0.0, rb))
            for half in range(2):
                ln = slice(128 * half, 128 * half + 128)
                t = [fv[2, r, 8 * j:8 * j + 8, ln] for j in range(2)]
                n1 = around(t[0], t[1], None, 1, sub)
                for j in range(2):
                    pre[NV + 2, r, 8 * j:8 * j + 8, ln] = 0.5 * (t[j] + n1[j])
            return carry
        lax.fori_loop(0, ROWS, step, 0, unroll=4)

        def mean_step(r, carry):
            pre[NV, r] = 0.5 * (fv[0, r] + fv[0, r + 1])
            return carry
        lax.fori_loop(0, ROWS - 1, mean_step, 0)
        pre[NV, ROWS - 1] = 0.5 * fv[0, ROWS - 1]

    for f in range(NV):
        raw_field(f)

    for d in FAR_FIRST:
        q_copy(d).wait_recv()

    @pl.when(has_prev)
    def _():
        for d in FAR_FIRST + (0,):
            q_up(d).wait_recv()

    @pl.when(has_next)
    def _():
        for d in FAR_FIRST + (0,):
            q_down(d).wait_recv()

    def z_sums(at):
        pair, quad = (at // 2) * 2, (at // 4) * 4
        s32 = zsum[pair] + zsum[pair + 1]
        s64 = (zsum[quad] + zsum[quad + 1]) + (zsum[quad + 2] + zsum[quad + 3])
        return s32, s64

    tall = (ROWS + 8, 128)
    wide = jnp.broadcast_to(width[0:1], tall)
    total = zsum[0]
    for i in range(1, NZ):
        total = total + zsum[i]
    gsum[g] = total

    def g_copy(d):
        return remote(gsum.at[g], gsum.at[g], g_send.at[d], g_recv.at[d], row, group(d))

    @pl.when(off_seam)
    def _():
        for d in G_ORDER:
            g_copy(d).start()

    def z_edge(at):
        s32, s64 = z_sums(at)
        return jnp.where(wide == 32, s32 * (1 / 32), s64 * (1 / 64))

    edge[4] = z_edge(jnp.where(z == 1, NZ - 1, 0))
    edge_up = remote(edge.at[4], edge.at[2], e_send.at[0], e_recv.at[0], row, group(1))
    edge_down = remote(edge.at[4], edge.at[3], e_send.at[1], e_recv.at[1], row, group(NG - 1))

    @pl.when(z == 1)
    def _():
        edge_up.start()

    @pl.when(z == NZ - 2)
    def _():
        edge_down.start()

    edge[0] = z_edge((z + NZ - 1) % NZ)
    edge[1] = z_edge((z + 1) % NZ)

    for copy in bulk[2 * EARLY:]:
        copy.start()

    raw_faces()

    seg, m = lane // 16, lane % 16
    is_even = seg % 2 == 0
    diff_even = jnp.zeros((8, 128), F32)
    diff_odd = jnp.zeros((8, 128), F32)
    for f in range(NV):
        t = jnp.where(low, diffusion[f:f + 1, 0:128], diffusion[f:f + 1, 128:256])
        t = pltpu.roll(jnp.broadcast_to(t, (8, 128)), (8 + 16 * f) % 128, 1) * (1.0 / 12.0)
        near_f = (lane - 16 * f + 2 + 128) % 128 < 20
        if f % 2 == 0:
            diff_even = jnp.where(near_f, t, diff_even)
        else:
            diff_odd = jnp.where(near_f, t, diff_odd)
    own = jnp.where(is_even, diff_even, diff_odd)
    out = jnp.where(is_even, diff_odd, diff_even)
    fluid = seg < NV
    zero = jnp.zeros((8, 128), F32)
    c0 = jnp.where(fluid, 1.0 - 90.0 * own, 0.5)
    c1 = jnp.where(fluid, 16.0 * own, zero)
    c2 = jnp.where(fluid, -own, zero)
    c_row = jnp.where(seg == NV, 0.5, zero)
    c_cell = jnp.where(seg == NV + 2, 0.5, zero)
    k1p = jnp.where(m % 8 == 0, zero, c1)
    k1n = jnp.where(m % 8 == 7, zero, c1 + jnp.where(seg == NV + 1, 0.5, zero))
    k2p = jnp.where(m % 8 < 2, zero, c2)
    k2n = jnp.where(m % 8 > 5, zero, c2)
    from_left = (seg + 7) % 8
    from_right = (seg + 1) % 8
    left_fluid, right_fluid = from_left < NV, from_right < NV
    s1p = jnp.where(jnp.logical_and(m == 0, left_fluid), 16.0 * out, zero)
    s2p = jnp.where(jnp.logical_and(m < 2, left_fluid), -out, zero)
    s1n = jnp.where(jnp.logical_and(m == 15, right_fluid), 16.0 * out, zero)
    s1n = jnp.where(jnp.logical_and(m == 15, from_right == NV + 1), 0.5, s1n)
    s2n = jnp.where(jnp.logical_and(m > 13, right_fluid), -out, zero)

    inner = (lane >= 8, lane < 120)

    @pl.when(has_prev)
    def _():
        for copy in up:
            copy.wait_recv()
        for f in range(NV):
            for half in range(2):
                ln = slice(128 * half, 128 * half + 128)
                diff = diffusion[f:f + 1, ln] * (1.0 / 12.0)
                for at in (slice(0, 8), slice(8, 16)):
                    b2, b1 = (jnp.where(inner[half], radial[f, i, at, ln], 0.0) for i in (0, 1))
                    pre[f, 0, at, ln] = pre[f, 0, at, ln] + diff * (16.0 * b1 - b2)
                    pre[f, 1, at, ln] = pre[f, 1, at, ln] - diff * b1

    @pl.when(has_next)
    def _():
        for copy in down:
            copy.wait_recv()
        for half in range(2):
            ln = slice(128 * half, 128 * half + 128)
            for at in (slice(0, 8), slice(8, 16)):
                for f in range(NV):
                    diff = diffusion[f:f + 1, ln] * (1.0 / 12.0)
                    b1, b2 = (jnp.where(inner[half], radial[f, i, at, ln], 0.0) for i in (2, 3))
                    e, e1 = ROWS - 1, ROWS - 2
                    pre[f, e, at, ln] = pre[f, e, at, ln] + diff * (16.0 * b1 - b2)
                    pre[f, e1, at, ln] = pre[f, e1, at, ln] - diff * b1
                b = jnp.where(inner[half], radial[NV, 2, at, ln], 0.0)
                pre[NV, ROWS - 1, at, ln] = pre[NV, ROWS - 1, at, ln] + 0.5 * b

    a1 = jnp.where(sub == 0, 16.0, zero)
    a2 = jnp.where(sub < 2, -1.0, zero)
    b1 = jnp.where(sub == 7, 16.0, zero)
    b2 = jnp.where(sub > 5, -1.0, zero)
    for f in range(NV):
        bulk[2 * f].wait_recv()
        bulk[2 * f + 1].wait_recv()
        diffs = [diffusion[f:f + 1, 128 * half:128 * half + 128] * (1.0 / 12.0) for half in range(2)]

        def step(r, carry):
            for half in range(2):
                ln = slice(128 * half, 128 * half + 128)
                h = jnp.where(inner[half], halo[f, r, :, ln], 0.0) * diffs[half]
                head = a1 * pltpu.roll(h, 1, 0) + a2 * pltpu.roll(h, 2, 0)
                tail = b1 * pltpu.roll(h, 7, 0) + b2 * pltpu.roll(h, 6, 0)
                pre[f, r, 0:8, ln] = pre[f, r, 0:8, ln] + head
                pre[f, r, 8:16, ln] = pre[f, r, 8:16, ln] + tail
            return carry
        lax.fori_loop(0, ROWS, step, 0, unroll=8)
    bulk[2 * NV].wait_recv()

    def face_step(r, carry):
        for half in range(2):
            ln = slice(128 * half, 128 * half + 128)
            h = pltpu.roll(halo[NV, r, :, ln], 7, 0)
            h = jnp.where(jnp.logical_and(inner[half], sub == 7), 0.5 * h, 0.0)
            pre[NV + 2, r, 8:16, ln] = pre[NV + 2, r, 8:16, ln] + h
        return carry
    lax.fori_loop(0, ROWS, face_step, 0, unroll=8)

    @pl.when(off_seam)
    def _():
        for d in G_ORDER:
            g_copy(d).wait_recv()

    @pl.when(z == 1)
    def _():
        edge_up.wait_recv()
        edge_up.wait_send()

    @pl.when(z == NZ - 2)
    def _():
        edge_down.wait_recv()
        edge_down.wait_send()

    edge_first.wait_recv()
    edge_last.wait_recv()

    whole = gsum[0]
    for i in range(1, NG):
        whole = whole + gsum[i]
    whole = whole * (1 / 1024)

    def g_means(at, small):
        pair, quad = (at // 2) * 2, (at // 4) * 4
        mean = jnp.where(wide == 128, gsum[at] * (1 / 128), small)
        mean = jnp.where(wide == 256, (gsum[pair] + gsum[pair + 1]) * (1 / 256), mean)
        four = (gsum[quad] + gsum[quad + 1]) + (gsum[quad + 2] + gsum[quad + 3])
        mean = jnp.where(wide == 512, four * (1 / 512), mean)
        return jnp.where(wide == 1024, whole, mean)

    s32, s64 = z_sums(z)
    mm[0] = g_means(g, jnp.where(wide == 32, s32 * (1 / 32), s64 * (1 / 64)))
    mm[1] = g_means(g, edge[0])
    mm[2] = g_means(g, edge[1])
    feed = remote(fed.at[0], fed.at[1], f_sem.at[0], f_sem.at[1], row, beside)

    @pl.when(feeder)
    def _():
        low_side = z == 1
        across = g_means(
            jnp.where(low_side, (g + NG - 1) % NG, (g + 1) % NG),
            jnp.where(low_side, edge[2], edge[3]),
        )
        fed[0, 0] = jnp.where(low_side, mm[1], mm[2])
        fed[0, 1] = jnp.where(low_side, across, mm[0])
        fed[0, 2] = jnp.where(low_side, mm[0], across)
        feed.start()

    @pl.when(at_seam)
    def _():
        feed.wait_recv()
        mm[...] = fed[1]

    mm[1, 0:ROWS] = jnp.where(wide[:ROWS] <= 16, last_in[...], mm[1, 0:ROWS])
    mm[2, 0:ROWS] = jnp.where(wide[:ROWS] <= 16, first_in[...], mm[2, 0:ROWS])
    narrow = width <= 16

    def differ(r, carry):
        mean = jnp.broadcast_to(mm[0, pl.ds(r, 1), :], (8, 128))
        for j in (0, 8):
            a = jnp.where(narrow, la[r, j:j + 8, :], mean)
            packed_out[r, j:j + 8, :] = a
            dd[r + 2, j:j + 8, :] = a - pp[r, j:j + 8, :]
        prev = jnp.broadcast_to(mm[1, pl.ds(r, 1), :], (8, 128))
        follow = jnp.broadcast_to(mm[2, pl.ds(r, 1), :], (8, 128))
        dd[r + 2, 16:24, :] = jnp.where(sub < 4, follow, prev)
        return carry

    lax.fori_loop(0, ROWS, differ, 0, unroll=8)

    for side, wait, which in ((has_prev, la_up, (0, 1)), (has_next, la_down, (2, 3))):
        @pl.when(side)
        def _():
            wait.wait_recv()
            for i in which:
                mean = jnp.broadcast_to(mm[0, ROWS + i:ROWS + i + 1, :], (8, 128))
                for j in (0, 8):
                    a = jnp.where(narrow, la_in[i, j:j + 8, :], mean)
                    dd[i if i < 2 else ROWS + i, j:j + 8, :] = a

        @pl.when(jnp.logical_not(side))
        def _():
            for i in which:
                dd[i if i < 2 else ROWS + i, 0:16, :] = jnp.zeros((16, 128), F32)

    def correct(r, carry):
        t = [dd[r + 2, 8 * j:8 * j + 8, :] for j in range(3)]
        n1, n2 = around(*t, 1, sub), around(*t, 2, sub)
        p1, p2 = around(*t, -1, sub), around(*t, -2, sub)
        for j in range(2):
            at = slice(8 * j, 8 * j + 8)
            d = t[j]
            below = dd[r + 3, at, :]
            near = (n1[j] + p1[j]) + (dd[r + 1, at, :] + below)
            far = (n2[j] + p2[j]) + (dd[r, at, :] + dd[r + 4, at, :])
            lp1, lp2 = pltpu.roll(d, 1, 1), pltpu.roll(d, 2, 1)
            ln1, ln2 = pltpu.roll(d, 127, 1), pltpu.roll(d, 126, 1)
            base = (c0 * d + c1 * near) + (c2 * far + c_row * below)
            base = base + (c_cell * n1[j] + k1p * lp1) + (k1n * ln1 + k2p * lp2) + k2n * ln2
            side = (s1p * lp1 + s2p * lp2) + (s1n * ln1 + s2n * ln2)
            even[r, at, :] = jnp.where(is_even, base, side)
            odd[r, at, :] = jnp.where(is_even, side, base)
        return carry

    lax.fori_loop(0, ROWS, correct, 0, unroll=4)

    for d in FAR_FIRST:
        q_copy(d).wait_send()

    @pl.when(off_seam)
    def _():
        for d in G_ORDER:
            g_copy(d).wait_send()

    pl.when(feeder)(feed.wait_send)
    for copy in bulk + [edge_first, edge_last]:
        copy.wait_send()

    @pl.when(has_prev)
    def _():
        la_down.wait_send()
        for copy in down:
            copy.wait_send()
        for d in range(NZ):
            q_down(d).wait_send()

    @pl.when(has_next)
    def _():
        la_up.wait_send()
        for copy in up:
            copy.wait_send()
        for d in range(NZ):
            q_up(d).wait_send()


def run_exchange(widths, hydro, face, diffusion):
    dma = pltpu.SemaphoreType.DMA
    packed = jax.ShapeDtypeStruct((ROWS, CELLS, 128), F32)
    return pl.pallas_call(
        exchange,
        out_shape=(jax.ShapeDtypeStruct((FIELDS, ROWS, CELLS, THETA), F32), packed, packed, packed),
        in_specs=[pl.BlockSpec(memory_space=pltpu.HBM)] * 4,
        out_specs=(pl.BlockSpec(memory_space=pltpu.VMEM),) * 4,
        scratch_shapes=[
            pltpu.VMEM((NV, ROWS + 4, CELLS, THETA), F32),
            pltpu.VMEM((NF, ROWS, CELLS, THETA), F32),
            pltpu.VMEM((NV + 1, ROWS, 8, THETA), F32),
            pltpu.VMEM((NV + 1, 4, CELLS, THETA), F32),
            pltpu.VMEM((ROWS, CELLS, 128), F32),
            pltpu.VMEM((ROWS, CELLS, 128), F32),
            pltpu.VMEM((NZ, ROWS + 8, 128), F32),
            pltpu.VMEM((NG, ROWS + 8, 128), F32),
            pltpu.VMEM((5, ROWS + 8, 128), F32),
            pltpu.VMEM((ROWS, 128), F32),
            pltpu.VMEM((ROWS, 128), F32),
            pltpu.VMEM((ROWS, 128), F32),
            pltpu.VMEM((ROWS, 128), F32),
            pltpu.VMEM((4, CELLS, 128), F32),
            pltpu.VMEM((ROWS + 4, CELLS + 8, 128), F32),
            pltpu.VMEM((3, ROWS + 8, 128), F32),
            pltpu.SMEM((16,), jnp.int32),
            pltpu.VMEM((NV, THETA), F32),
            dma((2,)),
            dma((8,)),
            dma((NZ,)), dma((NZ,)), dma((NZ,)), dma((NZ,)), dma((NZ,)), dma((NZ,)),
            dma((4,)), dma((4,)), dma((2,)), dma((2,)), dma((NG,)), dma((NG,)),
            dma((2 * NV + 1,)), dma((2 * NV + 1,)), dma((3,)), dma((3,)),
            pltpu.VMEM((2, 3, ROWS + 8, 128), F32), dma((2,)),
        ],
        compiler_params=pltpu.CompilerParams(
            collective_id=0, has_side_effects=True, vmem_limit_bytes=20 << 20
        ),
        name="exchange",
    )(*(pltpu.with_memory_space_constraint(x, pltpu.HBM) for x in (widths, hydro, face, diffusion)))


def update(pre, even, odd, packed, face, conserved, faces_out, co, fo, store_sem):
    lane = lanes((8, 128))

    def stores(f, part):
        at = pl.ds(PART * part, PART)
        out = [pltpu.make_async_copy(co.at[f, at], conserved.at[f, at], store_sem.at[f, part])]
        if f >= NV:
            k = f - NV
            out.append(pltpu.make_async_copy(fo.at[k, at], faces_out.at[k, at], store_sem.at[FIELDS + k, part]))
        return out

    order = (5, 6, 7, 0, 1, 2, 3, 4)
    for f in order:
        shift = (120 - 16 * f) % 128
        delta = even if f % 2 == 0 else odd

        def step(r, carry):
            for j in (0, 8):
                at = slice(j, j + 8)
                p = pltpu.roll(delta[r, at, :], shift, 1)
                co[f, r, at, 0:128] = pre[f, r, at, 0:128] + jnp.where(lane < 10, p, 0.0)
                co[f, r, at, 128:256] = pre[f, r, at, 128:256] + jnp.where(lane >= 118, p, 0.0)
                if f >= NV:
                    p = pltpu.roll(packed[r, at, :], shift, 1)
                    fo[f - NV, r, at, 0:128] = jnp.where(lane < 8, p, face[f - NV, r, at, 0:128])
                    fo[f - NV, r, at, 128:256] = jnp.where(lane >= 120, p, face[f - NV, r, at, 128:256])
            return carry

        for part in range(ROWS // PART):
            lax.fori_loop(PART * part, PART * part + PART, step, 0, unroll=8)
            for store in stores(f, part):
                store.start()

    for f in order:
        for part in range(ROWS // PART):
            for store in stores(f, part):
                store.wait()


def run_update(pre, even, odd, packed, face):
    return pl.pallas_call(
        update,
        out_shape=(
            jax.ShapeDtypeStruct((FIELDS, ROWS, CELLS, THETA), F32),
            jax.ShapeDtypeStruct((NF, ROWS, CELLS, THETA), F32),
        ),
        in_specs=[pl.BlockSpec(memory_space=pltpu.VMEM)] * 5,
        out_specs=(pl.BlockSpec(memory_space=pltpu.HBM), pl.BlockSpec(memory_space=pltpu.HBM)),
        scratch_shapes=[
            pltpu.VMEM((FIELDS, ROWS, CELLS, THETA), F32),
            pltpu.VMEM((NF, ROWS, CELLS, THETA), F32),
            pltpu.SemaphoreType.DMA((FIELDS + NF, ROWS // PART)),
        ],
        compiler_params=pltpu.CompilerParams(vmem_limit_bytes=16 << 20),
        name="update",
    )(pre, even, odd, packed, face)


def body(hydro, face, widths, diffusion):
    return run_update(*run_exchange(widths, hydro, face, diffusion), face)


def solution(mesh):
    spec = P(None, "row", "phi", None)
    return jax.shard_map(
        body, mesh=mesh, in_specs=(spec, spec, P(), P()), out_specs=(spec, spec), check_vma=False
    )
```
